512 devices in a mesh: obs: 64 (over z_hi, x, y), head: 8 (over z_lo, core).
Axes of the slice: x: 4, y: 8, z: 8 (z_hi: 2, z_lo: 4; z = z_hi * 4 + z_lo), core: 2. Of those that a mesh axis runs over, the one named last changes fastest.
Arguments:
- queries: bfloat16 [1024, 2048], P('obs', 'head'), may hold values from -6 to 6
- out_grad: bfloat16 [1024, 2048], P('obs', 'head'), may hold values from -6 to 6
- attn_out: bfloat16 [1024, 2048], P('obs', 'head'), may hold values from -6 to 6
- logsumexp: float32 [1024, 16], P('obs', 'head'), may hold values from 2.5 to 4.5
- keys: bfloat16 [24576, 2048], P('obs', 'head'), may hold values from -6 to 6
- values: bfloat16 [24576, 2048], P('obs', 'head'), may hold values from -6 to 6
- obs_counts: int32 [64], P('obs'), may hold values from 1 to 384, as said below
- query_weight: bfloat16 [2048, 2048], P(None, 'head'), may hold values from -0.125 to 0.125
Outputs:
- key_grad: bfloat16 [24576, 2048], P('obs', 'head')
- value_grad: bfloat16 [24576, 2048], P('obs', 'head')
- query_grad: bfloat16 [1024, 2048], P('obs', 'head')
- grid_grad: bfloat16 [1024, 2048], P('obs', 'head')
The draws below stay inside these ranges and needn't reach their ends.
Inputs may be any that keep to these rules, and one draw needn't show every extreme that they name: Each index of obs holds its tokens in its first obs_counts slots of 384; in every draw some index is full, with exactly 384.
All inputs are finite; a program needn't handle non-finite values.
Results may differ from the reference program's by a relative error of at most 0.0055.
Values may be sent and summed in bfloat16 or wider, within the bound.
A program may use at most 64 MiB of HBM per device.

```python
import math
import jax
import jax.numpy as jnp
from jax import lax

D = 2048
H = 16
DH = 128
TOK_DEV = 384
Q = 1024
NOBS = 24576
N_OBS = 64


def draw_obs_counts(key, part):
    key_level, key_jitter, key_full = jax.random.split(jax.random.fold_in(key, 17), 3)
    levels = jax.random.randint(key_level, (N_OBS,), 0, 4)
    base_counts = jnp.right_shift(jnp.full((N_OBS,), TOK_DEV, jnp.int32), levels.astype(jnp.int32))
    jitter = jax.random.randint(key_jitter, (N_OBS,), 0, base_counts // 4 + 1)
    full_index = jax.random.randint(key_full, (), 0, N_OBS)
    counts = jnp.where(jnp.arange(N_OBS, dtype=jnp.int32) == full_index, TOK_DEV, base_counts - jitter)
    return jnp.maximum(counts, 1).astype(jnp.int32)


def block_levels(rng, dims, cuts, smallest, largest):
    def one(dim, shards_of):
        heights = jax.random.uniform(jax.random.fold_in(jax.random.fold_in(rng, 6), dim), (shards_of,), jnp.float32, smallest / len(cuts), largest / len(cuts))
        return jnp.repeat(jnp.exp(heights), dims[dim] // shards_of).reshape((-1,) + (1,) * (len(dims) - dim - 1))

    level = one(*cuts[0])
    for cut in cuts[1:]:
        level = level * one(*cut)
    return level


def centred(key, shape, spread, most, pieces=(), kind=jnp.bfloat16):
    values = spread * jax.random.normal(key, shape, jnp.float32)
    if pieces:
        values = values * block_levels(key, shape, pieces, -0.22, 0.18)
    return jnp.clip(values, -most, most).astype(kind)


def setup_inputs(seed: int = 0) -> dict:
    seeds = jax.random.split(jax.random.key(seed), 9)
    return {
        "queries": centred(seeds[0], (Q, D), 1.0, 6.0, ((0, 64), (1, 8))),
        "out_grad": centred(seeds[1], (Q, D), 1.0, 6.0, ((0, 64), (1, 8))),
        "attn_out": centred(seeds[2], (Q, D), 1.0, 6.0, ((0, 64), (1, 8))),
        "logsumexp": jnp.clip(2.5 + 2.0 * jax.random.uniform(seeds[3], (Q, H), jnp.float32) ** block_levels(seeds[3], (Q, H), ((0, 64), (1, 8)), -0.2, 0.2), 2.5, 4.5),
        "keys": centred(seeds[4], (NOBS, D), 1.0, 6.0, ((0, 64), (1, 8))),
        "values": centred(seeds[5], (NOBS, D), 1.0, 6.0, ((0, 64), (1, 8))),
        "obs_counts": draw_obs_counts(jax.random.fold_in(seeds[8], 71), 0),
        "query_weight": centred(seeds[7], (D, D), D ** -0.5, 0.125, ((1, 8),)),
    }


def reference(queries, out_grad, attn_out, logsumexp, keys, values, obs_counts, query_weight):
    softmax_scale = 1.0 / math.sqrt(DH)
    query_heads = queries.reshape(Q, H, DH).transpose(1, 0, 2)
    grad_heads = out_grad.reshape(Q, H, DH).transpose(1, 0, 2)
    delta = lax.optimization_barrier(jnp.sum(out_grad.astype(jnp.float32).reshape(Q, H, DH) * attn_out.astype(jnp.float32).reshape(Q, H, DH), axis=2))
    key_heads = keys.reshape(N_OBS, TOK_DEV, H, DH).transpose(2, 0, 1, 3)
    value_heads = values.reshape(N_OBS, TOK_DEV, H, DH).transpose(2, 0, 1, 3)
    live = (jnp.arange(TOK_DEV, dtype=jnp.int32)[None, :] < obs_counts[:, None]).astype(jnp.float32)

    def one_head(inputs):
        query_now, grad_now, lse_now, delta_now, key_now, value_now = inputs

        def key_block(query_acc, blocks):
            key_rows, value_rows, live_rows = blocks
            scores = jnp.dot(query_now, key_rows.T, preferred_element_type=jnp.float32) * softmax_scale
            probs = jnp.exp(scores - lse_now[:, None]) * live_rows[None, :]
            value_part = jnp.dot(probs.astype(jnp.bfloat16).T, grad_now, preferred_element_type=jnp.float32)
            dprobs = jnp.dot(grad_now, value_rows.T, preferred_element_type=jnp.float32)
            dscores = (probs * (dprobs - delta_now[:, None])).astype(jnp.bfloat16)
            key_part = jnp.dot(dscores.T, query_now, preferred_element_type=jnp.float32) * softmax_scale
            query_acc = query_acc + jnp.dot(dscores, key_rows, preferred_element_type=jnp.float32) * softmax_scale
            return (query_acc, (key_part, value_part))
        query_acc, parts = lax.scan(key_block, jnp.zeros((Q, DH), jnp.float32), (key_now, value_now, live))
        return (query_acc, parts[0], parts[1])
    query_sum, key_part, value_part = lax.map(one_head, (query_heads, grad_heads, logsumexp.T, delta.T, key_heads, value_heads))
    key_grad = key_part.transpose(1, 2, 0, 3).reshape(NOBS, D).astype(jnp.bfloat16)
    value_grad = value_part.transpose(1, 2, 0, 3).reshape(NOBS, D).astype(jnp.bfloat16)
    query_grad = query_sum.transpose(1, 0, 2).reshape(Q, D).astype(jnp.bfloat16)
    grid_grad = jnp.dot(query_grad, query_weight.T, preferred_element_type=jnp.float32).astype(jnp.bfloat16)
    return (key_grad, value_grad, query_grad, grid_grad)
```

```python
import math

import jax
import jax.numpy as jnp
from jax import lax
from jax.experimental import pallas as pl
from jax.experimental.pallas import tpu as pltpu
from jax.sharding import PartitionSpec as P

MESH = pl.DeviceIdType.MESH
DH = 128
NZ, NX, NY = 2, 4, 8
HEADS = 8
ROWS = 16
TOK = 384
COL = 256
BLK = NY * ROWS
SCALE = 1.0 / math.sqrt(DH)
LOG2E = math.log2(math.e)


def ring_offset(i, n):
    d = i // 2 + 1
    odd = i % 2
    return (1 - odd) * d + odd * (n - d)


def kernel(
    q_hbm, g_hbm, o_hbm, lse_hbm, k_hbm, v_hbm, cnt, w_hbm,
    kg_hbm, vg_hbm, qg_out, gg_out,
    qg, att, lse_v, kb, vb, kt, wb,
    ldb, ldg, dk, dv, dqs, dqo, rs1, redb, rs2, gs, gr, kob, vob,
    sem_in, sem_out, s_z, s_y, s_yl, s_x, s_xl, s_r1, s_r2, s_g,
    r_q, r_l, r_lg, r_r1, r_r2, r_g,
):
    obs = lax.axis_index("obs")
    head = lax.axis_index("head")
    z = obs // (NX * NY)
    x = (obs // NY) % NX
    y = obs % NY
    zo = 1 - z

    def dev(zz, xx, yy):
        return ((zz * NX + xx) * NY + yy, head)

    def slot(zz, xx, yy):
        return (zz * NX + xx) * NY + yy

    def xpeer(i):
        return (x + ring_offset(i, NX)) % NX

    def xsource(i):
        return (x + NX - ring_offset(i, NX)) % NX

    def ypeer(i):
        return (y + ring_offset(i, NY)) % NY

    def remote(src, dst, ssem, rsem, device):
        return pltpu.make_async_remote_copy(
            src_ref=src, dst_ref=dst, send_sem=ssem, recv_sem=rsem,
            device_id=device, device_id_type=MESH)

    me = slot(z, x, y)
    loads = [
        pltpu.make_async_copy(q_hbm, qg.at[me, :, pl.ds(0, COL)], sem_in.at[0]),
        pltpu.make_async_copy(g_hbm, qg.at[me, :, pl.ds(COL, COL)], sem_in.at[1]),
        pltpu.make_async_copy(o_hbm, att, sem_in.at[2]),
        pltpu.make_async_copy(lse_hbm, lse_v, sem_in.at[3]),
        pltpu.make_async_copy(k_hbm, kb, sem_in.at[4]),
        pltpu.make_async_copy(v_hbm, vb, sem_in.at[5]),
        pltpu.make_async_copy(w_hbm, wb, sem_in.at[6]),
    ]
    for c in loads:
        c.start()

    barrier = pltpu.get_barrier_semaphore()

    def hello(device):
        pl.semaphore_signal(barrier, inc=1, device_id=device, device_id_type=MESH)

    hello(dev(zo, x, y))

    def hello_y(i, c):
        hello(dev(z, x, ypeer(i)))
        hello(dev(zo, x, ypeer(i)))
        return c

    lax.fori_loop(0, NY - 1, hello_y, 0)

    def hello_x(i, c):
        hello(dev(z, xpeer(i), y))
        return c

    lax.fori_loop(0, NX - 1, hello_x, 0)

    def hello_h(i, c):
        hello((obs, (head + 1 + i) % HEADS))
        return c

    lax.fori_loop(0, HEADS - 1, hello_h, 0)

    for c in loads[:4]:
        c.wait()

    row = lax.broadcasted_iota(jnp.int32, (ROWS, BLK), 0)
    lane = lax.broadcasted_iota(jnp.int32, (ROWS, BLK), 1)
    mine = lane == row + y * ROWS
    own = z * NY + y
    for h in range(2):
        og = qg[me, :, COL + h * DH : COL + (h + 1) * DH].astype(jnp.float32)
        ao = att[:, h * DH : (h + 1) * DH].astype(jnp.float32)
        delta = jnp.sum(og * ao, axis=1, keepdims=True)
        lse = lse_v[:, h : h + 1] * LOG2E
        ldb[own, h : h + 1, :] = jnp.sum(jnp.where(mine, lse, 0.0), axis=0, keepdims=True)
        ldb[own, 2 + h : 3 + h, :] = jnp.sum(jnp.where(mine, delta, 0.0), axis=0, keepdims=True)

    pl.semaphore_wait(barrier, 1 + 2 * (NY - 1) + NX - 1 + HEADS - 1)

    def z_copy(k):
        if k == 0:
            return remote(qg.at[me], qg.at[me], s_z.at[0], r_q.at[me], dev(zo, x, y))
        return remote(ldb.at[own], ldb.at[own], s_z.at[1], r_l.at[own], dev(zo, x, y))

    def y_copies(zz, i):
        s = slot(zz, x, y)
        l = zz * NY + y
        n = zz * (NY - 1) + i
        to = dev(z, x, ypeer(i))
        return (remote(qg.at[s], qg.at[s], s_y.at[n], r_q.at[s], to),
                remote(ldb.at[l], ldb.at[l], s_yl.at[n], r_l.at[l], to))

    def x_copy(zz, yy, i):
        s = slot(zz, x, yy)
        n = (zz * NY + yy) * (NX - 1) + i
        return remote(qg.at[s], qg.at[s], s_x.at[n], r_q.at[s], dev(z, xpeer(i), y))

    def xl_copy(zz, i):
        n = zz * NX + x
        return remote(ldg.at[n], ldg.at[n], s_xl.at[zz * (NX - 1) + i], r_lg.at[n], dev(z, xpeer(i), y))

    def wait_q(s):
        remote(qg.at[s], qg.at[s], s_z.at[0], r_q.at[s], dev(zo, x, y)).wait_recv()

    def wait_l(l):
        remote(ldb.at[l], ldb.at[l], s_z.at[1], r_l.at[l], dev(zo, x, y)).wait_recv()

    def wait_lg(n):
        remote(ldg.at[n], ldg.at[n], s_z.at[1], r_lg.at[n], dev(zo, x, y)).wait_recv()

    def spread_y(zz):
        def body(i, c):
            for copy in y_copies(zz, i):
                copy.start()
            return c
        lax.fori_loop(0, NY - 1, body, 0)

    def spread_x(zz, yy):
        def body(i, c):
            x_copy(zz, yy, i).start()
            return c
        lax.fori_loop(0, NX - 1, body, 0)

    def pass_on(zz):
        def body(i, c):
            yy = ypeer(i)
            wait_q(slot(zz, x, yy))
            spread_x(zz, yy)
            return c
        lax.fori_loop(0, NY - 1, body, 0)

        def body_l(i, c):
            wait_l(zz * NY + ypeer(i))
            return c
        lax.fori_loop(0, NY - 1, body_l, 0)
        total = ldb[zz * NY]
        for k in range(1, NY):
            total = total + ldb[zz * NY + k]
        ldg[zz * NX + x] = total

        def body_g(i, c):
            xl_copy(zz, i).start()
            return c
        lax.fori_loop(0, NX - 1, body_g, 0)

    z_copy(0).start()
    z_copy(1).start()
    spread_y(z)
    spread_x(z, y)

    for c in loads[4:]:
        c.wait()
    for h in range(2):
        kt[h] = kb[:, h * DH : (h + 1) * DH].astype(jnp.float32).T.astype(jnp.bfloat16)
    dk[...] = jnp.zeros_like(dk)
    dv[...] = jnp.zeros_like(dv)
    live = lax.broadcasted_iota(jnp.int32, (TOK, BLK), 0) < cnt[0]

    def adjoint(zz, xx):
        base = slot(zz, xx, 0)
        parts = []
        for h in range(2):
            cols = slice(h * DH, (h + 1) * DH)
            qh = qg[pl.ds(base, NY), :, h * DH : (h + 1) * DH].reshape(BLK, DH)
            gh = qg[pl.ds(base, NY), :, COL + h * DH : COL + (h + 1) * DH].reshape(BLK, DH)
            lse = ldg[zz * NX + xx, h : h + 1, :]
            delta = ldg[zz * NX + xx, 2 + h : 3 + h, :]
            nt = (((1,), (1,)), ((), ()))
            scores = lax.dot_general(kb[:, cols], qh, nt, preferred_element_type=jnp.float32)
            dprobs = lax.dot_general(vb[:, cols], gh, nt, preferred_element_type=jnp.float32)
            probs = jnp.where(live, jnp.exp2(scores * (SCALE * LOG2E) - lse), 0.0)
            dscores = (probs * (dprobs - delta)).astype(jnp.bfloat16)
            dv[:, cols] += jnp.dot(probs.astype(jnp.bfloat16), gh, preferred_element_type=jnp.float32)
            dk[:, cols] += jnp.dot(dscores, qh, preferred_element_type=jnp.float32)
            dqt = jnp.dot(kt[h], dscores, preferred_element_type=jnp.float32)
            parts.append(dqt.T)
        return parts

    def own_group(zz):
        parts = adjoint(zz, x)
        for h in range(2):
            dqo[zz, :, h * DH : (h + 1) * DH] = parts[h]

    def r1_copy(zz, i):
        n = zz * (NX - 1) + i
        return remote(dqs.at[n], rs1.at[n], s_r1.at[n], r_r1.at[n], dev(z, xpeer(i), y))

    def other_groups(zz):
        def body(i, c):
            xx = xpeer(i)

            def arrive(yy, c2):
                wait_q(slot(zz, xx, yy))
                return c2
            lax.fori_loop(0, NY, arrive, 0)
            wait_lg(zz * NX + xx)
            parts = adjoint(zz, xx)
            n = zz * (NX - 1) + i
            for h in range(2):
                dqs[n, :, :, h * DH : (h + 1) * DH] = parts[h].astype(jnp.bfloat16).reshape(NY, ROWS, DH)
            r1_copy(zz, i).start()
            return c
        lax.fori_loop(0, NX - 1, body, 0)

    def r2_copy(zz, yy):
        n = zz * NY + yy
        return remote(redb.at[n], rs2.at[own], s_r2.at[n], r_r2.at[own], dev(zz, x, yy))

    def reduce_x(zz):
        for i in range(NX - 1):
            r1_copy(zz, i).wait_recv()
        total = dqo[zz]
        for i in range(NX - 1):
            total = total + rs1[zz * (NX - 1) + i].reshape(BLK, COL).astype(jnp.float32)
        redb[pl.ds(zz * NY, NY)] = total.astype(jnp.bfloat16).reshape(NY, ROWS, COL)

    pass_on(z)
    own_group(z)
    wait_q(slot(zo, x, y))
    wait_l(zo * NY + y)
    spread_y(zo)
    spread_x(zo, y)
    other_groups(z)
    pass_on(zo)
    own_group(zo)
    reduce_x(z)

    def near(i, c):
        r2_copy(z, ypeer(i)).start()
        return c
    lax.fori_loop(0, NY - 1, near, 0)
    rs2[own] = redb[own]
    other_groups(zo)
    kob[...] = (dk[...] * SCALE).astype(jnp.bfloat16)
    vob[...] = dv[...].astype(jnp.bfloat16)
    outs = [pltpu.make_async_copy(kob, kg_hbm, sem_out.at[0]),
            pltpu.make_async_copy(vob, vg_hbm, sem_out.at[1])]
    for c in outs:
        c.start()
    reduce_x(zo)

    def far(i, c):
        r2_copy(zo, (y + i) % NY).start()
        return c
    lax.fori_loop(0, NY, far, 0)

    def landed_near(i, c):
        l = z * NY + ypeer(i)
        remote(rs2.at[l], rs2.at[l], s_z.at[0], r_r2.at[l], dev(zo, x, y)).wait_recv()
        return c
    lax.fori_loop(0, NY - 1, landed_near, 0)

    def landed_far(i, c):
        l = zo * NY + i
        remote(rs2.at[l], rs2.at[l], s_z.at[0], r_r2.at[l], dev(zo, x, y)).wait_recv()
        return c
    lax.fori_loop(0, NY, landed_far, 0)

    query_half = (jnp.sum(rs2[...].astype(jnp.float32), axis=0) * SCALE).astype(jnp.bfloat16)
    qg_out[...] = query_half

    def g_copy(j):
        return remote(gs.at[j], gr.at[head], s_g.at[j], r_g.at[head], (obs, j))

    def grid_block(i, c):
        j = (head + 1 + i) % HEADS
        part = lax.dot_general(query_half, wb[pl.ds(j * COL, COL), :], (((1,), (1,)), ((), ())),
                               preferred_element_type=jnp.float32)
        gs[j] = part
        g_copy(j).start()
        return c
    lax.fori_loop(0, HEADS - 1, grid_block, 0)
    gr[head] = lax.dot_general(query_half, wb[pl.ds(head * COL, COL), :], (((1,), (1,)), ((), ())),
                               preferred_element_type=jnp.float32)

    def grid_landed(i, c):
        j = (head + 1 + i) % HEADS
        remote(gr.at[j], gr.at[j], s_g.at[j], r_g.at[j], (obs, j)).wait_recv()
        return c
    lax.fori_loop(0, HEADS - 1, grid_landed, 0)
    gg_out[...] = jnp.sum(gr[...], axis=0).astype(jnp.bfloat16)

    z_copy(0).wait_send()
    z_copy(1).wait_send()

    def sent_y(i, c):
        for zz in (z, zo):
            for copy in y_copies(zz, i):
                copy.wait_send()
        return c
    lax.fori_loop(0, NY - 1, sent_y, 0)

    def sent_x(i, c):
        def inner(yy, c2):
            x_copy(0, yy, i).wait_send()
            x_copy(1, yy, i).wait_send()
            return c2
        lax.fori_loop(0, NY, inner, 0)
        for zz in range(NZ):
            xl_copy(zz, i).wait_send()
            r1_copy(zz, i).wait_send()
        return c
    lax.fori_loop(0, NX - 1, sent_x, 0)

    def sent_near(i, c):
        r2_copy(z, ypeer(i)).wait_send()
        return c
    lax.fori_loop(0, NY - 1, sent_near, 0)

    def sent_far(i, c):
        r2_copy(zo, i).wait_send()
        return c
    lax.fori_loop(0, NY, sent_far, 0)

    def sent_g(i, c):
        g_copy((head + 1 + i) % HEADS).wait_send()
        return c
    lax.fori_loop(0, HEADS - 1, sent_g, 0)
    for c in outs:
        c.wait()


def on_device(queries, out_grad, attn_out, logsumexp, keys, values, obs_counts, query_weight):
    bf, f32 = jnp.bfloat16, jnp.float32
    anywhere = pl.BlockSpec(memory_space=pl.ANY)
    vmem = pl.BlockSpec(memory_space=pltpu.VMEM)
    dma = pltpu.SemaphoreType.DMA
    blocks = NZ * NX * NY
    return pl.pallas_call(
        kernel,
        name="adjoint",
        out_shape=(
            jax.ShapeDtypeStruct((TOK, COL), bf),
            jax.ShapeDtypeStruct((TOK, COL), bf),
            jax.ShapeDtypeStruct((ROWS, COL), bf),
            jax.ShapeDtypeStruct((ROWS, COL), bf),
        ),
        in_specs=[anywhere] * 6 + [pl.BlockSpec(memory_space=pltpu.SMEM), anywhere],
        out_specs=(anywhere, anywhere, vmem, vmem),
        scratch_shapes=[
            pltpu.VMEM((blocks, ROWS, 2 * COL), bf),
            pltpu.VMEM((ROWS, COL), bf),
            pltpu.VMEM((ROWS, 2), f32),
            pltpu.VMEM((TOK, COL), bf),
            pltpu.VMEM((TOK, COL), bf),
            pltpu.VMEM((2, DH, TOK), bf),
            pltpu.VMEM((HEADS * COL, COL), bf),
            pltpu.VMEM((NZ * NY, 4, BLK), f32),
            pltpu.VMEM((NZ * NX, 4, BLK), f32),
            pltpu.VMEM((TOK, COL), f32),
            pltpu.VMEM((TOK, COL), f32),
            pltpu.VMEM((NZ * (NX - 1), NY, ROWS, COL), bf),
            pltpu.VMEM((NZ, BLK, COL), f32),
            pltpu.VMEM((NZ * (NX - 1), NY, ROWS, COL), bf),
            pltpu.VMEM((NZ * NY, ROWS, COL), bf),
            pltpu.VMEM((NZ * NY, ROWS, COL), bf),
            pltpu.VMEM((HEADS, ROWS, COL), f32),
            pltpu.VMEM((HEADS, ROWS, COL), f32),
            pltpu.VMEM((TOK, COL), bf),
            pltpu.VMEM((TOK, COL), bf),
            dma((7,)), dma((2,)), dma((2,)), dma((NZ * (NY - 1),)), dma((NZ * (NY - 1),)),
            dma((NZ * NY * (NX - 1),)), dma((NZ * (NX - 1),)), dma((NZ * (NX - 1),)),
            dma((NZ * NY,)), dma((HEADS,)),
            dma((blocks,)), dma((NZ * NY,)), dma((NZ * NX,)), dma((NZ * (NX - 1),)),
            dma((NZ * NY,)), dma((HEADS,)),
        ],
        compiler_params=pltpu.CompilerParams(collective_id=0, has_side_effects=True),
    )(queries, out_grad, attn_out, logsumexp, keys, values, obs_counts, query_weight)


def solution(mesh):
    in_specs = (
        P("obs", "head"),
        P("obs", "head"),
        P("obs", "head"),
        P("obs", "head"),
        P("obs", "head"),
        P("obs", "head"),
        P("obs"),
        P(None, "head"),
    )
    out_specs = (P("obs", "head"), P("obs", "head"), P("obs", "head"), P("obs", "head"))
    return jax.shard_map(
        on_device, mesh=mesh, in_specs=in_specs, out_specs=out_specs, check_vma=False
    )
```

```python
import math

import jax
import jax.numpy as jnp
from jax import lax
from jax.experimental import pallas as pl
from jax.experimental.pallas import tpu as pltpu
from jax.sharding import PartitionSpec as P

MESH = pl.DeviceIdType.MESH
DH = 128
NZ, NX, NY = 2, 4, 8
HEADS = 8
ROWS = 16
TOK = 384
COL = 256
BLK = NY * ROWS
SCALE = 1.0 / math.sqrt(DH)
LOG2E = math.log2(math.e)


def ring_offset(i, n):
    d = i // 2 + 1
    odd = i % 2
    return (1 - odd) * d + odd * (n - d)


def kernel(
    q_hbm, g_hbm, o_hbm, lse_hbm, k_hbm, v_hbm, cnt, w_hbm,
    kob, vob, qg_out, gg_out,
    qg, att, lse_v, kb, vb, kt, wb,
    ldb, ldg, dk, dv, dqs, dqo, rs1, redb, rs2, gs, gr,
    sem_in, s_z, s_y, s_yl, s_x, s_xl, s_r1, s_r2, s_g,
    r_q, r_l, r_lg, r_r1, r_r2, r_g,
):
    obs = lax.axis_index("obs")
    head = lax.axis_index("head")
    z = obs // (NX * NY)
    x = (obs // NY) % NX
    y = obs % NY
    zo = 1 - z

    def dev(zz, xx, yy):
        return ((zz * NX + xx) * NY + yy, head)

    def slot(zz, xx, yy):
        return (zz * NX + xx) * NY + yy

    def xpeer(i):
        return (x + ring_offset(i, NX)) % NX

    def xsource(i):
        return (x + NX - ring_offset(i, NX)) % NX

    def ypeer(i):
        return (y + ring_offset(i, NY)) % NY

    def remote(src, dst, ssem, rsem, device):
        return pltpu.make_async_remote_copy(
            src_ref=src, dst_ref=dst, send_sem=ssem, recv_sem=rsem,
            device_id=device, device_id_type=MESH)

    me = slot(z, x, y)
    loads = [
        pltpu.make_async_copy(q_hbm, qg.at[me, :, pl.ds(0, COL)], sem_in.at[0]),
        pltpu.make_async_copy(g_hbm, qg.at[me, :, pl.ds(COL, COL)], sem_in.at[1]),
        pltpu.make_async_copy(o_hbm, att, sem_in.at[2]),
        pltpu.make_async_copy(lse_hbm, lse_v, sem_in.at[3]),
        pltpu.make_async_copy(k_hbm, kb, sem_in.at[4]),
        pltpu.make_async_copy(v_hbm, vb, sem_in.at[5]),
        pltpu.make_async_copy(w_hbm, wb, sem_in.at[6]),
    ]
    for c in loads:
        c.start()

    barrier = pltpu.get_barrier_semaphore()

    def hello(device):
        pl.semaphore_signal(barrier, inc=1, device_id=device, device_id_type=MESH)

    hello(dev(zo, x, y))

    def hello_y(i, c):
        hello(dev(z, x, ypeer(i)))
        return c

    lax.fori_loop(0, NY - 1, hello_y, 0)

    def hello_x(i, c):
        hello(dev(z, xpeer(i), y))
        return c

    lax.fori_loop(0, NX - 1, hello_x, 0)

    def hello_h(i, c):
        hello((obs, (head + 1 + i) % HEADS))
        return c

    lax.fori_loop(0, HEADS - 1, hello_h, 0)

    for c in loads[:4]:
        c.wait()

    row = lax.broadcasted_iota(jnp.int32, (ROWS, BLK), 0)
    lane = lax.broadcasted_iota(jnp.int32, (ROWS, BLK), 1)
    mine = lane == row + y * ROWS
    my_lanes = lax.broadcasted_iota(jnp.int32, (1, BLK), 1) // ROWS == y
    own = z * NY + y
    for h in range(2):
        og = qg[me, :, COL + h * DH : COL + (h + 1) * DH].astype(jnp.float32)
        ao = att[:, h * DH : (h + 1) * DH].astype(jnp.float32)
        delta = jnp.sum(og * ao, axis=1, keepdims=True)
        lse = jnp.concatenate([lse_v[h : h + 1, :] * LOG2E] * NY, axis=1)
        ldb[own, h : h + 1, :] = jnp.where(my_lanes, lse, 0.0)
        ldb[own, 2 + h : 3 + h, :] = jnp.sum(jnp.where(mine, delta, 0.0), axis=0, keepdims=True)

    pl.semaphore_wait(barrier, 1 + NY - 1 + NX - 1 + HEADS - 1)

    def z_copy(k):
        if k == 0:
            return remote(qg.at[me], qg.at[me], s_z.at[0], r_q.at[me], dev(zo, x, y))
        return remote(ldb.at[own], ldb.at[own], s_z.at[1], r_l.at[own], dev(zo, x, y))

    def y_copies(zz, i):
        s = slot(zz, x, y)
        l = zz * NY + y
        n = zz * (NY - 1) + i
        to = dev(z, x, ypeer(i))
        return (remote(qg.at[s], qg.at[s], s_y.at[n], r_q.at[s], to),
                remote(ldb.at[l], ldb.at[l], s_yl.at[n], r_l.at[l], to))

    def x_copy(zz, yy, i):
        s = slot(zz, x, yy)
        n = (zz * NY + yy) * (NX - 1) + i
        return remote(qg.at[s], qg.at[s], s_x.at[n], r_q.at[s], dev(z, xpeer(i), y))

    def xl_copy(zz, i):
        n = zz * NX + x
        return remote(ldg.at[n], ldg.at[n], s_xl.at[zz * (NX - 1) + i], r_lg.at[n], dev(z, xpeer(i), y))

    def wait_q(s):
        remote(qg.at[s], qg.at[s], s_z.at[0], r_q.at[s], dev(zo, x, y)).wait_recv()

    def wait_l(l):
        remote(ldb.at[l], ldb.at[l], s_z.at[1], r_l.at[l], dev(zo, x, y)).wait_recv()

    def wait_lg(n):
        remote(ldg.at[n], ldg.at[n], s_z.at[1], r_lg.at[n], dev(zo, x, y)).wait_recv()

    def spread_y(zz):
        def body(i, c):
            for copy in y_copies(zz, i):
                copy.start()
            return c
        lax.fori_loop(0, NY - 1, body, 0)

    def spread_x(zz, yy):
        def body(i, c):
            x_copy(zz, yy, i).start()
            return c
        lax.fori_loop(0, NX - 1, body, 0)

    def pass_on(zz):
        def body(i, c):
            yy = ypeer(i)
            wait_q(slot(zz, x, yy))
            spread_x(zz, yy)
            return c
        lax.fori_loop(0, NY - 1, body, 0)

        def body_l(i, c):
            wait_l(zz * NY + ypeer(i))
            return c
        lax.fori_loop(0, NY - 1, body_l, 0)
        total = ldb[zz * NY]
        for k in range(1, NY):
            total = total + ldb[zz * NY + k]
        ldg[zz * NX + x] = total

        def body_g(i, c):
            xl_copy(zz, i).start()
            return c
        lax.fori_loop(0, NX - 1, body_g, 0)

    z_copy(0).start()
    z_copy(1).start()
    spread_y(z)
    spread_x(z, y)

    for c in loads[4:]:
        c.wait()
    for h in range(2):
        kt[h] = kb[:, h * DH : (h + 1) * DH].astype(jnp.float32).T.astype(jnp.bfloat16)
    dk[...] = jnp.zeros_like(dk)
    dv[...] = jnp.zeros_like(dv)
    live = lax.broadcasted_iota(jnp.int32, (TOK, BLK), 0) < cnt[0]

    def adjoint(zz, xx):
        base = slot(zz, xx, 0)
        parts = []
        for h in range(2):
            cols = slice(h * DH, (h + 1) * DH)
            qh = qg[pl.ds(base, NY), :, h * DH : (h + 1) * DH].reshape(BLK, DH)
            gh = qg[pl.ds(base, NY), :, COL + h * DH : COL + (h + 1) * DH].reshape(BLK, DH)
            lse = ldg[zz * NX + xx, h : h + 1, :]
            delta = ldg[zz * NX + xx, 2 + h : 3 + h, :]
            nt = (((1,), (1,)), ((), ()))
            scores = lax.dot_general(kb[:, cols], qh, nt, preferred_element_type=jnp.float32)
            dprobs = lax.dot_general(vb[:, cols], gh, nt, preferred_element_type=jnp.float32)
            probs = jnp.where(live, jnp.exp2(scores * (SCALE * LOG2E) - lse), 0.0)
            dscores = (probs * (dprobs - delta)).astype(jnp.bfloat16)
            dv[:, cols] += jnp.dot(probs.astype(jnp.bfloat16), gh, preferred_element_type=jnp.float32)
            dk[:, cols] += jnp.dot(dscores, qh, preferred_element_type=jnp.float32)
            dqt = jnp.dot(kt[h], dscores, preferred_element_type=jnp.float32)
            parts.append(dqt.T)
        return parts

    def own_group(zz):
        parts = adjoint(zz, x)
        for h in range(2):
            dqo[zz, :, h * DH : (h + 1) * DH] = parts[h]

    def r1_copy(zz, i):
        n = zz * (NX - 1) + i
        return remote(dqs.at[n], rs1.at[n], s_r1.at[n], r_r1.at[n], dev(z, xpeer(i), y))

    def other_groups(zz, first, last):
        def body(i, c):
            xx = xpeer(i)

            def arrive(k, c2):
                wait_q(slot(zz, xx, k))
                return c2

            lax.fori_loop(0, NY, arrive, 0)
            wait_lg(zz * NX + xx)
            parts = adjoint(zz, xx)
            n = zz * (NX - 1) + i
            for h in range(2):
                dqs[n, :, :, h * DH : (h + 1) * DH] = parts[h].astype(jnp.bfloat16).reshape(NY, ROWS, DH)
            r1_copy(zz, i).start()
            return c
        lax.fori_loop(first, last, body, 0)

    def r2_copy(zz, yy):
        n = zz * NY + yy
        return remote(redb.at[n], rs2.at[own], s_r2.at[n], r_r2.at[own], dev(zz, x, yy))

    def reduce_x(zz):
        for i in range(NX - 1):
            r1_copy(zz, i).wait_recv()
        total = dqo[zz]
        for i in range(NX - 1):
            total = total + rs1[zz * (NX - 1) + i].reshape(BLK, COL).astype(jnp.float32)
        redb[pl.ds(zz * NY, NY)] = total.astype(jnp.bfloat16).reshape(NY, ROWS, COL)

    pass_on(z)
    wait_q(slot(zo, x, y))
    wait_l(zo * NY + y)
    spread_y(zo)
    spread_x(zo, y)
    pass_on(zo)
    own_group(z)
    own_group(zo)
    other_groups(z, 0, 2)
    other_groups(zo, 0, 2)
    other_groups(z, 2, 3)
    other_groups(zo, 2, 3)
    reduce_x(z)

    def near(i, c):
        r2_copy(z, ypeer(i)).start()
        return c
    lax.fori_loop(0, NY - 1, near, 0)
    rs2[own] = redb[own]
    kob[...] = (dk[...] * SCALE).astype(jnp.bfloat16)
    vob[...] = dv[...].astype(jnp.bfloat16)
    reduce_x(zo)

    def far(i, c):
        r2_copy(zo, (y + i) % NY).start()
        return c
    lax.fori_loop(0, NY, far, 0)

    def landed_near(i, c):
        l = z * NY + ypeer(i)
        remote(rs2.at[l], rs2.at[l], s_z.at[0], r_r2.at[l], dev(zo, x, y)).wait_recv()
        return c
    lax.fori_loop(0, NY - 1, landed_near, 0)

    def landed_far(i, c):
        l = zo * NY + i
        remote(rs2.at[l], rs2.at[l], s_z.at[0], r_r2.at[l], dev(zo, x, y)).wait_recv()
        return c
    lax.fori_loop(0, NY, landed_far, 0)

    query_half = (jnp.sum(rs2[...].astype(jnp.float32), axis=0) * SCALE).astype(jnp.bfloat16)
    qg_out[...] = query_half

    def g_copy(j):
        return remote(gs.at[j], gr.at[head], s_g.at[j], r_g.at[head], (obs, j))

    parts = lax.dot_general(query_half, wb[...], (((1,), (1,)), ((), ())), preferred_element_type=jnp.float32)
    for j in range(HEADS):
        gs[j] = parts[:, j * COL : (j + 1) * COL]

    def grid_send(i, c):
        g_copy((head + 1 + i) % HEADS).start()
        return c
    lax.fori_loop(0, HEADS - 1, grid_send, 0)
    gr[head] = gs[head]

    def grid_landed(i, c):
        j = (head + 1 + i) % HEADS
        remote(gr.at[j], gr.at[j], s_g.at[j], r_g.at[j], (obs, j)).wait_recv()
        return c
    lax.fori_loop(0, HEADS - 1, grid_landed, 0)
    gg_out[...] = jnp.sum(gr[...], axis=0).astype(jnp.bfloat16)

    z_copy(0).wait_send()
    z_copy(1).wait_send()

    def sent_y(i, c):
        for zz in (z, zo):
            for copy in y_copies(zz, i):
                copy.wait_send()
        return c
    lax.fori_loop(0, NY - 1, sent_y, 0)

    def sent_x(i, c):
        def inner(yy, c2):
            x_copy(0, yy, i).wait_send()
            x_copy(1, yy, i).wait_send()
            return c2
        lax.fori_loop(0, NY, inner, 0)
        for zz in range(NZ):
            xl_copy(zz, i).wait_send()
            r1_copy(zz, i).wait_send()
        return c
    lax.fori_loop(0, NX - 1, sent_x, 0)

    def sent_near(i, c):
        r2_copy(z, ypeer(i)).wait_send()
        return c
    lax.fori_loop(0, NY - 1, sent_near, 0)

    def sent_far(i, c):
        r2_copy(zo, i).wait_send()
        return c
    lax.fori_loop(0, NY, sent_far, 0)

    def sent_g(i, c):
        g_copy((head + 1 + i) % HEADS).wait_send()
        return c
    lax.fori_loop(0, HEADS - 1, sent_g, 0)


def finish(kob, vob, qgo, ggo, kg_hbm, vg_hbm, qg_hbm, gg_hbm, sem):
    pairs = ((qgo, qg_hbm), (ggo, gg_hbm), (kob, kg_hbm), (vob, vg_hbm))
    copies = [pltpu.make_async_copy(a, b, sem.at[i]) for i, (a, b) in enumerate(pairs)]
    for c in copies:
        c.start()
    for c in copies:
        c.wait()


def on_device(queries, out_grad, attn_out, logsumexp, keys, values, obs_counts, query_weight):
    bf, f32 = jnp.bfloat16, jnp.float32
    anywhere = pl.BlockSpec(memory_space=pl.ANY)
    vmem = pl.BlockSpec(memory_space=pltpu.VMEM)
    dma = pltpu.SemaphoreType.DMA
    blocks = NZ * NX * NY
    shapes = ((TOK, COL), (TOK, COL), (ROWS, COL), (ROWS, COL))
    held = pl.pallas_call(
        kernel,
        name="adjoint",
        out_shape=tuple(pltpu.VMEM(shape, bf) for shape in shapes),
        in_specs=[anywhere] * 6 + [pl.BlockSpec(memory_space=pltpu.SMEM), anywhere],
        out_specs=(vmem,) * 4,
        scratch_shapes=[
            pltpu.VMEM((blocks, ROWS, 2 * COL), bf),
            pltpu.VMEM((ROWS, COL), bf),
            pltpu.VMEM((2, ROWS), f32),
            pltpu.VMEM((TOK, COL), bf),
            pltpu.VMEM((TOK, COL), bf),
            pltpu.VMEM((2, DH, TOK), bf),
            pltpu.VMEM((HEADS * COL, COL), bf),
            pltpu.VMEM((NZ * NY, 4, BLK), f32),
            pltpu.VMEM((NZ * NX, 4, BLK), f32),
            pltpu.VMEM((TOK, COL), f32),
            pltpu.VMEM((TOK, COL), f32),
            pltpu.VMEM((NZ * (NX - 1), NY, ROWS, COL), bf),
            pltpu.VMEM((NZ, BLK, COL), f32),
            pltpu.VMEM((NZ * (NX - 1), NY, ROWS, COL), bf),
            pltpu.VMEM((NZ * NY, ROWS, COL), bf),
            pltpu.VMEM((NZ * NY, ROWS, COL), bf),
            pltpu.VMEM((HEADS, ROWS, COL), f32),
            pltpu.VMEM((HEADS, ROWS, COL), f32),
            dma((7,)), dma((2,)), dma((NZ * (NY - 1),)), dma((NZ * (NY - 1),)),
            dma((NZ * NY * (NX - 1),)), dma((NZ * (NX - 1),)), dma((NZ * (NX - 1),)),
            dma((NZ * NY,)), dma((HEADS,)),
            dma((blocks,)), dma((NZ * NY,)), dma((NZ * NX,)), dma((NZ * (NX - 1),)),
            dma((NZ * NY,)), dma((HEADS,)),
        ],
        compiler_params=pltpu.CompilerParams(collective_id=0, has_side_effects=True),
    )(queries, out_grad, attn_out, logsumexp.T, keys, values, obs_counts, query_weight)
    return pl.pallas_call(
        finish,
        name="finish",
        out_shape=tuple(jax.ShapeDtypeStruct(shape, bf) for shape in shapes),
        in_specs=[vmem] * 4,
        out_specs=(anywhere,) * 4,
        scratch_shapes=[dma((4,))],
    )(*[pltpu.with_memory_space_constraint(a, pltpu.VMEM) for a in held])


def solution(mesh):
    in_specs = (
        P("obs", "head"),
        P("obs", "head"),
        P("obs", "head"),
        P("obs", "head"),
        P("obs", "head"),
        P("obs", "head"),
        P("obs"),
        P(None, "head"),
    )
    out_specs = (P("obs", "head"), P("obs", "head"), P("obs", "head"), P("obs", "head"))
    return jax.shard_map(
        on_device, mesh=mesh, in_specs=in_specs, out_specs=out_specs, check_vma=False
    )
```

```python
import math

import jax
import jax.numpy as jnp
from jax import lax
from jax.experimental import pallas as pl
from jax.experimental.pallas import tpu as pltpu
from jax.sharding import PartitionSpec as P

MESH = pl.DeviceIdType.MESH
DH = 128
NZ, NX, NY = 2, 4, 8
HEADS = 8
ROWS = 16
TOK = 384
COL = 256
BLK = NY * ROWS
SCALE = 1.0 / math.sqrt(DH)
LOG2E = math.log2(math.e)


def ring_offset(i, n):
    d = i // 2 + 1
    odd = i % 2
    return (1 - odd) * d + odd * (n - d)


def kernel(
    q_hbm, g_hbm, o_hbm, lse_hbm, k_hbm, v_hbm, cnt, w_hbm,
    kob, vob, qg_out, gg_out,
    qg, att, lse_v, kb, vb, kt, wb,
    ldb, ldg, dk, dv, dqs, dqo, rs1, redb, rs2, gs, gr,
    sem_in, s_z, s_y, s_yl, s_x, s_xl, s_r1, s_r2, s_g,
    r_q, r_x, r_l, r_lg, r_r1, r_r2, r_g,
):
    obs = lax.axis_index("obs")
    head = lax.axis_index("head")
    z = obs // (NX * NY)
    x = (obs // NY) % NX
    y = obs % NY
    zo = 1 - z

    def dev(zz, xx, yy):
        return ((zz * NX + xx) * NY + yy, head)

    def slot(zz, xx, yy):
        return (zz * NX + xx) * NY + yy

    def xpeer(i):
        return (x + ring_offset(i, NX)) % NX

    def xsource(i):
        return (x + NX - ring_offset(i, NX)) % NX

    def ypeer(i):
        return (y + ring_offset(i, NY)) % NY

    def remote(src, dst, ssem, rsem, device):
        return pltpu.make_async_remote_copy(
            src_ref=src, dst_ref=dst, send_sem=ssem, recv_sem=rsem,
            device_id=device, device_id_type=MESH)

    me = slot(z, x, y)
    loads = [
        pltpu.make_async_copy(q_hbm, qg.at[me, :, pl.ds(0, COL)], sem_in.at[0]),
        pltpu.make_async_copy(g_hbm, qg.at[me, :, pl.ds(COL, COL)], sem_in.at[1]),
        pltpu.make_async_copy(o_hbm, att, sem_in.at[2]),
        pltpu.make_async_copy(lse_hbm, lse_v, sem_in.at[3]),
        pltpu.make_async_copy(k_hbm, kb, sem_in.at[4]),
        pltpu.make_async_copy(v_hbm, vb, sem_in.at[5]),
        pltpu.make_async_copy(w_hbm, wb, sem_in.at[6]),
    ]
    for c in loads:
        c.start()

    barrier = pltpu.get_barrier_semaphore()

    def hello(device):
        pl.semaphore_signal(barrier, inc=1, device_id=device, device_id_type=MESH)

    hello(dev(zo, x, y))

    def hello_y(i, c):
        hello(dev(z, x, ypeer(i)))
        return c

    lax.fori_loop(0, NY - 1, hello_y, 0)

    def hello_x(i, c):
        hello(dev(z, xpeer(i), y))
        return c

    lax.fori_loop(0, NX - 1, hello_x, 0)

    def hello_h(i, c):
        hello((obs, (head + 1 + i) % HEADS))
        return c

    lax.fori_loop(0, HEADS - 1, hello_h, 0)

    for c in loads[:2]:
        c.wait()
    own = z * NY + y
    pl.semaphore_wait(barrier, 1 + NY - 1 + NX - 1 + HEADS - 1)

    def z_copy(k):
        if k == 0:
            return remote(qg.at[me], qg.at[me], s_z.at[0], r_q.at[z * NY + y], dev(zo, x, y))
        return remote(ldb.at[own], ldb.at[own], s_z.at[1], r_l.at[own], dev(zo, x, y))

    def y_copies(zz, i):
        s = slot(zz, x, y)
        l = zz * NY + y
        to = dev(z, x, ypeer(i))
        return (remote(qg.at[s], qg.at[s], s_y.at[zz], r_q.at[l], to),
                remote(ldb.at[l], ldb.at[l], s_yl.at[zz], r_l.at[l], to))

    def strip(zz, xx):
        return qg.at[pl.ds(slot(zz, xx, 0), NY)]

    def row_copy(zz, i):
        return remote(strip(zz, x), strip(zz, x), s_x.at[zz * (NX - 1) + i], r_x.at[zz * NX + x], dev(z, xpeer(i), y))

    def x_copy(zz, yy, i):
        s = slot(zz, x, yy)
        return remote(qg.at[s], qg.at[s], s_x.at[zz * (NX - 1) + i], r_x.at[zz * NX + x], dev(z, xpeer(i), y))

    def xl_copy(zz, i):
        n = zz * NX + x
        return remote(ldg.at[n], ldg.at[n], s_xl.at[zz * (NX - 1) + i], r_lg.at[n], dev(z, xpeer(i), y))

    def wait_q(zz, yy):
        s = slot(zz, x, yy)
        remote(qg.at[s], qg.at[s], s_z.at[0], r_q.at[zz * NY + yy], dev(zo, x, y)).wait_recv()

    def wait_row(zz, xx):
        remote(strip(zz, xx), strip(zz, xx), s_x.at[0], r_x.at[zz * NX + xx], dev(z, xx, y)).wait_recv()

    def wait_l(l):
        remote(ldb.at[l], ldb.at[l], s_z.at[1], r_l.at[l], dev(zo, x, y)).wait_recv()

    def wait_lg(n):
        remote(ldg.at[n], ldg.at[n], s_z.at[1], r_lg.at[n], dev(zo, x, y)).wait_recv()

    def spread_y(zz, which):
        def body(i, c):
            y_copies(zz, i)[which].start()
            return c
        lax.fori_loop(0, NY - 1, body, 0)

    def spread_x(zz, yy):
        def body(i, c):
            x_copy(zz, yy, i).start()
            return c
        lax.fori_loop(0, NX - 1, body, 0)

    def rows_in(zz, pieces):
        def body(i, c):
            yy = ypeer(i)
            wait_q(zz, yy)
            if pieces:
                spread_x(zz, yy)
            return c
        lax.fori_loop(0, NY - 1, body, 0)
        if not pieces:
            for i in range(NX - 1):
                row_copy(zz, i).start()

        def body_l(i, c):
            wait_l(zz * NY + ypeer(i))
            return c
        lax.fori_loop(0, NY - 1, body_l, 0)
        total = ldb[zz * NY]
        for k in range(1, NY):
            total = total + ldb[zz * NY + k]
        ldg[zz * NX + x] = total

        def body_g(i, c):
            xl_copy(zz, i).start()
            return c
        lax.fori_loop(0, NX - 1, body_g, 0)

    z_copy(0).start()
    spread_y(z, 0)
    spread_x(z, y)

    for c in loads[2:4]:
        c.wait()

    row = lax.broadcasted_iota(jnp.int32, (ROWS, BLK), 0)
    lane = lax.broadcasted_iota(jnp.int32, (ROWS, BLK), 1)
    mine = lane == row + y * ROWS
    my_lanes = lax.broadcasted_iota(jnp.int32, (1, BLK), 1) // ROWS == y
    for h in range(2):
        og = qg[me, :, COL + h * DH : COL + (h + 1) * DH].astype(jnp.float32)
        ao = att[:, h * DH : (h + 1) * DH].astype(jnp.float32)
        delta = jnp.sum(og * ao, axis=1, keepdims=True)
        lse = jnp.concatenate([lse_v[h : h + 1, :] * LOG2E] * NY, axis=1)
        ldb[own, h : h + 1, :] = jnp.where(my_lanes, lse, 0.0)
        ldb[own, 2 + h : 3 + h, :] = jnp.sum(jnp.where(mine, delta, 0.0), axis=0, keepdims=True)

    z_copy(1).start()
    spread_y(z, 1)

    for c in loads[4:]:
        c.wait()
    for h in range(2):
        kt[h] = kb[:, h * DH : (h + 1) * DH].astype(jnp.float32).T.astype(jnp.bfloat16)
    dk[...] = jnp.zeros_like(dk)
    dv[...] = jnp.zeros_like(dv)
    live = lax.broadcasted_iota(jnp.int32, (TOK, BLK), 0) < cnt[0]

    def adjoint(zz, xx):
        base = slot(zz, xx, 0)
        parts = []
        for h in range(2):
            cols = slice(h * DH, (h + 1) * DH)
            qh = qg[pl.ds(base, NY), :, h * DH : (h + 1) * DH].reshape(BLK, DH)
            gh = qg[pl.ds(base, NY), :, COL + h * DH : COL + (h + 1) * DH].reshape(BLK, DH)
            lse = ldg[zz * NX + xx, h : h + 1, :]
            delta = ldg[zz * NX + xx, 2 + h : 3 + h, :]
            nt = (((1,), (1,)), ((), ()))
            scores = lax.dot_general(kb[:, cols], qh, nt, preferred_element_type=jnp.float32)
            dprobs = lax.dot_general(vb[:, cols], gh, nt, preferred_element_type=jnp.float32)
            probs = jnp.where(live, jnp.exp2(scores * (SCALE * LOG2E) - lse), 0.0)
            dscores = (probs * (dprobs - delta)).astype(jnp.bfloat16)
            dv[:, cols] += jnp.dot(probs.astype(jnp.bfloat16), gh, preferred_element_type=jnp.float32)
            dk[:, cols] += jnp.dot(dscores, qh, preferred_element_type=jnp.float32)
            dqt = jnp.dot(kt[h], dscores, preferred_element_type=jnp.float32)
            parts.append(dqt.T)
        return parts

    def own_group(zz):
        parts = adjoint(zz, x)
        for h in range(2):
            dqo[zz, :, h * DH : (h + 1) * DH] = parts[h]

    def r1_copy(zz, i):
        n = zz * (NX - 1) + i
        return remote(dqs.at[n], rs1.at[n], s_r1.at[n], r_r1.at[n], dev(z, xpeer(i), y))

    def other_groups(zz, first, last):
        def body(i, c):
            xx = xpeer(i)

            wait_row(zz, xx)
            wait_lg(zz * NX + xx)
            parts = adjoint(zz, xx)
            n = zz * (NX - 1) + i
            for h in range(2):
                dqs[n, :, :, h * DH : (h + 1) * DH] = parts[h].astype(jnp.bfloat16).reshape(NY, ROWS, DH)
            r1_copy(zz, i).start()
            return c
        lax.fori_loop(first, last, body, 0)

    def r2_copy(zz, yy):
        n = zz * NY + yy
        n_to = jnp.where(zz == z, y, NY)
        return remote(redb.at[n], rs2.at[own], s_r2.at[zz], r_r2.at[n_to], dev(zz, x, yy))

    def reduce_x(zz):
        for i in range(NX - 1):
            r1_copy(zz, i).wait_recv()
        total = dqo[zz]
        for i in range(NX - 1):
            total = total + rs1[zz * (NX - 1) + i].reshape(BLK, COL).astype(jnp.float32)
        redb[pl.ds(zz * NY, NY)] = total.astype(jnp.bfloat16).reshape(NY, ROWS, COL)

    rows_in(z, True)
    wait_q(zo, y)
    spread_y(zo, 0)
    wait_l(zo * NY + y)
    spread_y(zo, 1)
    spread_x(zo, y)
    own_group(z)
    rows_in(zo, True)
    other_groups(z, 2, 3)
    other_groups(z, 0, 2)
    own_group(zo)
    other_groups(zo, 2, 3)
    other_groups(zo, 0, 2)
    reduce_x(z)

    def near(i, c):
        r2_copy(z, ypeer(i)).start()
        return c
    lax.fori_loop(0, NY - 1, near, 0)
    rs2[own] = redb[own]
    kob[...] = (dk[...] * SCALE).astype(jnp.bfloat16)
    vob[...] = dv[...].astype(jnp.bfloat16)
    reduce_x(zo)

    def far(i, c):
        r2_copy(zo, (y + i) % NY).start()
        return c
    lax.fori_loop(0, NY, far, 0)

    z_copy(0).wait_send()
    z_copy(1).wait_send()
    for zz in range(NZ):
        blocks = qg.at[pl.ds(0, NY - 1)]
        remote(blocks, blocks, s_y.at[zz], r_q.at[0], dev(zo, x, y)).wait_send()
        rows = ldb.at[pl.ds(0, NY - 1)]
        remote(rows, rows, s_yl.at[zz], r_l.at[0], dev(zo, x, y)).wait_send()
        for i in range(NX - 1):
            row_copy(zz, i).wait_send()
            xl_copy(zz, i).wait_send()
            r1_copy(zz, i).wait_send()

    def landed_near(i, c):
        l = z * NY + ypeer(i)
        remote(rs2.at[l], rs2.at[l], s_z.at[0], r_r2.at[ypeer(i)], dev(z, x, ypeer(i))).wait_recv()
        return c
    lax.fori_loop(0, NY - 1, landed_near, 0)
    far_part = rs2.at[pl.ds(zo * NY, NY)]
    remote(far_part, far_part, s_z.at[0], r_r2.at[NY], dev(zo, x, y)).wait_recv()

    query_half = (jnp.sum(rs2[...].astype(jnp.float32), axis=0) * SCALE).astype(jnp.bfloat16)
    qg_out[...] = query_half

    def g_copy(j):
        return remote(gs.at[j], gr.at[head], s_g.at[0], r_g.at[head], (obs, j))

    parts = lax.dot_general(query_half, wb[...], (((1,), (1,)), ((), ())), preferred_element_type=jnp.float32)
    for j in range(HEADS):
        gs[j] = parts[:, j * COL : (j + 1) * COL].astype(jnp.bfloat16)

    def grid_send(i, c):
        g_copy((head + 1 + i) % HEADS).start()
        return c
    lax.fori_loop(0, HEADS - 1, grid_send, 0)
    gr[head] = gs[head]

    near_part = redb.at[pl.ds(0, NY - 1)]
    far_sent = redb.at[pl.ds(0, NY)]
    remote(near_part, near_part, s_r2.at[z], r_r2.at[0], dev(zo, x, y)).wait_send()
    remote(far_sent, far_sent, s_r2.at[zo], r_r2.at[0], dev(zo, x, y)).wait_send()

    def grid_landed(i, c):
        j = (head + 1 + i) % HEADS
        remote(gr.at[j], gr.at[j], s_g.at[0], r_g.at[j], (obs, j)).wait_recv()
        return c
    lax.fori_loop(0, HEADS - 1, grid_landed, 0)
    gg_out[...] = jnp.sum(gr[...].astype(jnp.float32), axis=0).astype(jnp.bfloat16)

    pieces = gs.at[pl.ds(0, HEADS - 1)]
    remote(pieces, pieces, s_g.at[0], r_g.at[0], (obs, head)).wait_send()


def finish(kob, vob, qgo, ggo, kg_hbm, vg_hbm, qg_hbm, gg_hbm, sem):
    pairs = ((qgo, qg_hbm), (ggo, gg_hbm), (kob, kg_hbm), (vob, vg_hbm))
    copies = [pltpu.make_async_copy(a, b, sem.at[i]) for i, (a, b) in enumerate(pairs)]
    for c in copies:
        c.start()
    for c in copies:
        c.wait()


def on_device(queries, out_grad, attn_out, logsumexp, keys, values, obs_counts, query_weight):
    bf, f32 = jnp.bfloat16, jnp.float32
    anywhere = pl.BlockSpec(memory_space=pl.ANY)
    vmem = pl.BlockSpec(memory_space=pltpu.VMEM)
    dma = pltpu.SemaphoreType.DMA
    blocks = NZ * NX * NY
    shapes = ((TOK, COL), (TOK, COL), (ROWS, COL), (ROWS, COL))
    held = pl.pallas_call(
        kernel,
        name="adjoint",
        out_shape=tuple(pltpu.VMEM(shape, bf) for shape in shapes),
        in_specs=[anywhere] * 6 + [pl.BlockSpec(memory_space=pltpu.SMEM), anywhere],
        out_specs=(vmem,) * 4,
        scratch_shapes=[
            pltpu.VMEM((blocks, ROWS, 2 * COL), bf),
            pltpu.VMEM((ROWS, COL), bf),
            pltpu.VMEM((2, ROWS), f32),
            pltpu.VMEM((TOK, COL), bf),
            pltpu.VMEM((TOK, COL), bf),
            pltpu.VMEM((2, DH, TOK), bf),
            pltpu.VMEM((HEADS * COL, COL), bf),
            pltpu.VMEM((NZ * NY, 4, BLK), f32),
            pltpu.VMEM((NZ * NX, 4, BLK), f32),
            pltpu.VMEM((TOK, COL), f32),
            pltpu.VMEM((TOK, COL), f32),
            pltpu.VMEM((NZ * (NX - 1), NY, ROWS, COL), bf),
            pltpu.VMEM((NZ, BLK, COL), f32),
            pltpu.VMEM((NZ * (NX - 1), NY, ROWS, COL), bf),
            pltpu.VMEM((NZ * NY, ROWS, COL), bf),
            pltpu.VMEM((NZ * NY, ROWS, COL), bf),
            pltpu.VMEM((HEADS, ROWS, COL), bf),
            pltpu.VMEM((HEADS, ROWS, COL), bf),
            dma((7,)), dma((2,)), dma((NZ,)), dma((NZ,)), dma((NZ * (NX - 1),)), dma((NZ * (NX - 1),)),
            dma((NZ * (NX - 1),)), dma((NZ,)), dma((1,)),
            dma((NZ * NY,)), dma((NZ * NX,)), dma((NZ * NY,)), dma((NZ * NX,)), dma((NZ * (NX - 1),)),
            dma((NY + 1,)), dma((HEADS,)),
        ],
        compiler_params=pltpu.CompilerParams(collective_id=0, has_side_effects=True),
    )(queries, out_grad, attn_out, logsumexp.T, keys, values, obs_counts, query_weight)
    return pl.pallas_call(
        finish,
        name="finish",
        out_shape=tuple(jax.ShapeDtypeStruct(shape, bf) for shape in shapes),
        in_specs=[vmem] * 4,
        out_specs=(anywhere,) * 4,
        scratch_shapes=[dma((4,))],
    )(*[pltpu.with_memory_space_constraint(a, pltpu.VMEM) for a in held])


def solution(mesh):
    in_specs = (
        P("obs", "head"),
        P("obs", "head"),
        P("obs", "head"),
        P("obs", "head"),
        P("obs", "head"),
        P("obs", "head"),
        P("obs"),
        P(None, "head"),
    )
    out_specs = (P("obs", "head"), P("obs", "head"), P("obs", "head"), P("obs", "head"))
    return jax.shard_map(
        on_device, mesh=mesh, in_specs=in_specs, out_specs=out_specs, check_vma=False
    )
```

```python
import math

import jax
import jax.numpy as jnp
from jax import lax
from jax.experimental import pallas as pl
from jax.experimental.pallas import tpu as pltpu
from jax.sharding import PartitionSpec as P

MESH = pl.DeviceIdType.MESH
DH = 128
NZ, NX, NY = 2, 4, 8
HEADS = 8
ROWS = 16
TOK = 384
COL = 256
BLK = NY * ROWS
SCALE = 1.0 / math.sqrt(DH)
LOG2E = math.log2(math.e)


def ring_offset(i, n):
    d = i // 2 + 1
    odd = i % 2
    return (1 - odd) * d + odd * (n - d)


def kernel(
    q_hbm, g_hbm, o_hbm, lse_hbm, k_hbm, v_hbm, cnt, w_hbm,
    kob, vob, qg_out, gg_out,
    qg, att, lse_v, kb, vb, kt, wb,
    ldb, ldg, pall, sall, dqs, dqo, rs1, redb, rs2, gs, gr,
    sem_in, s_z, s_y, s_yl, s_x, s_f, s_xl, s_r1, s_r2, s_g,
    r_q, r_x, r_f, r_l, r_lg, r_r1, r_r2, r_g,
):
    obs = lax.axis_index("obs")
    head = lax.axis_index("head")
    z = obs // (NX * NY)
    x = (obs // NY) % NX
    y = obs % NY
    zo = 1 - z

    def dev(zz, xx, yy):
        return ((zz * NX + xx) * NY + yy, head)

    def slot(zz, xx, yy):
        return (zz * NX + xx) * NY + yy

    def xpeer(i):
        return (x + ring_offset(i, NX)) % NX

    def xsource(i):
        return (x + NX - ring_offset(i, NX)) % NX

    def ypeer(i):
        return (y + ring_offset(i, NY)) % NY

    def remote(src, dst, ssem, rsem, device):
        return pltpu.make_async_remote_copy(
            src_ref=src, dst_ref=dst, send_sem=ssem, recv_sem=rsem,
            device_id=device, device_id_type=MESH)

    me = slot(z, x, y)
    loads = [
        pltpu.make_async_copy(q_hbm, qg.at[me, :, pl.ds(0, COL)], sem_in.at[0]),
        pltpu.make_async_copy(g_hbm, qg.at[me, :, pl.ds(COL, COL)], sem_in.at[1]),
        pltpu.make_async_copy(o_hbm, att, sem_in.at[2]),
        pltpu.make_async_copy(lse_hbm, lse_v, sem_in.at[3]),
        pltpu.make_async_copy(k_hbm, kb, sem_in.at[4]),
        pltpu.make_async_copy(v_hbm, vb, sem_in.at[5]),
        pltpu.make_async_copy(w_hbm, wb, sem_in.at[6]),
    ]
    for c in loads:
        c.start()

    barrier = pltpu.get_barrier_semaphore()

    def hello(device):
        pl.semaphore_signal(barrier, inc=1, device_id=device, device_id_type=MESH)

    hello(dev(zo, x, y))

    def hello_y(i, c):
        hello(dev(z, x, ypeer(i)))
        return c

    lax.fori_loop(0, NY - 1, hello_y, 0)

    def hello_x(i, c):
        hello(dev(z, xpeer(i), y))
        return c

    lax.fori_loop(0, NX - 1, hello_x, 0)

    def hello_h(i, c):
        hello((obs, (head + 1 + i) % HEADS))
        return c

    lax.fori_loop(0, HEADS - 1, hello_h, 0)

    for c in loads[:2]:
        c.wait()
    own = z * NY + y
    pl.semaphore_wait(barrier, 1 + NY - 1 + NX - 1 + HEADS - 1)

    def z_copy(k):
        if k == 0:
            return remote(qg.at[me], qg.at[me], s_z.at[0], r_q.at[z * NY + y], dev(zo, x, y))
        return remote(ldb.at[own], ldb.at[own], s_z.at[1], r_l.at[own], dev(zo, x, y))

    def y_copies(zz, i):
        s = slot(zz, x, y)
        l = zz * NY + y
        to = dev(z, x, ypeer(i))
        return (remote(qg.at[s], qg.at[s], s_y.at[zz], r_q.at[l], to),
                remote(ldb.at[l], ldb.at[l], s_yl.at[zz], r_l.at[l], to))

    def strip(zz, xx):
        return qg.at[pl.ds(slot(zz, xx, 0), NY)]

    def row_copy(zz, i):
        return remote(strip(zz, x), strip(zz, x), s_x.at[zz * (NX - 1) + i], r_x.at[zz * NX + x], dev(z, xpeer(i), y))

    def x_copy(zz, yy, i):
        s = slot(zz, x, yy)
        return remote(qg.at[s], qg.at[s], s_x.at[zz * (NX - 1) + i], r_x.at[zz * NX + x], dev(z, xpeer(i), y))

    def xl_copy(zz, i):
        n = zz * NX + x
        return remote(ldg.at[n], ldg.at[n], s_xl.at[zz * (NX - 1) + i], r_lg.at[n], dev(z, xpeer(i), y))

    def wait_q(zz, yy):
        s = slot(zz, x, yy)
        remote(qg.at[s], qg.at[s], s_z.at[0], r_q.at[zz * NY + yy], dev(zo, x, y)).wait_recv()

    def wait_row(zz, xx):
        remote(strip(zz, xx), strip(zz, xx), s_x.at[0], r_x.at[zz * NX + xx], dev(z, xx, y)).wait_recv()

    def wait_l(l):
        remote(ldb.at[l], ldb.at[l], s_z.at[1], r_l.at[l], dev(zo, x, y)).wait_recv()

    def wait_lg(n):
        remote(ldg.at[n], ldg.at[n], s_z.at[1], r_lg.at[n], dev(zo, x, y)).wait_recv()

    def spread_y(zz, which):
        def body(i, c):
            y_copies(zz, i)[which].start()
            return c
        lax.fori_loop(0, NY - 1, body, 0)

    def spread_x(zz, yy, sides):
        def body(i, c):
            x_copy(zz, yy, i).start()
            return c
        lax.fori_loop(0, sides, body, 0)

    xf = (x + NX // 2) % NX

    def far_copy():
        return remote(qg.at[me], qg.at[me], s_f.at[0], r_f.at[y], dev(z, xf, y))

    def far_y_copy(i):
        s = slot(z, xf, y)
        return remote(qg.at[s], qg.at[s], s_f.at[1], r_f.at[y], dev(z, x, ypeer(i)))

    def wait_far(yy):
        s = slot(z, xf, yy)
        remote(qg.at[s], qg.at[s], s_f.at[0], r_f.at[yy], dev(z, xf, y)).wait_recv()

    def spread_far():
        wait_far(y)

        def body(i, c):
            far_y_copy(i).start()
            return c
        lax.fori_loop(0, NY - 1, body, 0)

    def rows_in(zz, sides, first, last):
        def body(i, c):
            yy = ypeer(i)
            wait_q(zz, yy)
            spread_x(zz, yy, sides)
            return c
        lax.fori_loop(first, last, body, 0)

    def rows_done(zz):
        def body_l(i, c):
            wait_l(zz * NY + ypeer(i))
            return c
        lax.fori_loop(0, NY - 1, body_l, 0)
        total = ldb[zz * NY]
        for k in range(1, NY):
            total = total + ldb[zz * NY + k]
        ldg[zz * NX + x] = total

        def body_g(i, c):
            xl_copy(zz, i).start()
            return c
        lax.fori_loop(0, NX - 1, body_g, 0)

    z_copy(0).start()
    spread_y(z, 0)
    far_copy().start()
    spread_x(z, y, 2)

    for c in loads[2:4]:
        c.wait()

    row = lax.broadcasted_iota(jnp.int32, (ROWS, BLK), 0)
    lane = lax.broadcasted_iota(jnp.int32, (ROWS, BLK), 1)
    mine = lane == row + y * ROWS
    my_lanes = lax.broadcasted_iota(jnp.int32, (1, BLK), 1) // ROWS == y
    for h in range(2):
        og = qg[me, :, COL + h * DH : COL + (h + 1) * DH].astype(jnp.float32)
        ao = att[:, h * DH : (h + 1) * DH].astype(jnp.float32)
        delta = jnp.sum(og * ao, axis=1, keepdims=True)
        lse = jnp.concatenate([lse_v[h : h + 1, :] * LOG2E] * NY, axis=1)
        ldb[own, h : h + 1, :] = jnp.where(my_lanes, lse, 0.0)
        ldb[own, 2 + h : 3 + h, :] = jnp.sum(jnp.where(mine, delta, 0.0), axis=0, keepdims=True)

    z_copy(1).start()
    spread_y(z, 1)

    for c in loads[4:]:
        c.wait()
    for h in range(2):
        kt[h] = kb[:, h * DH : (h + 1) * DH].astype(jnp.float32).T.astype(jnp.bfloat16)
    live = lax.broadcasted_iota(jnp.int32, (TOK, BLK), 0) < cnt[0]

    def adjoint(zz, xx):
        base = slot(zz, xx, 0)
        at = pl.ds(pl.multiple_of(base * ROWS, BLK), BLK)
        parts = []
        for h in range(2):
            cols = slice(h * DH, (h + 1) * DH)
            qh = qg[pl.ds(base, NY), :, h * DH : (h + 1) * DH].reshape(BLK, DH)
            gh = qg[pl.ds(base, NY), :, COL + h * DH : COL + (h + 1) * DH].reshape(BLK, DH)
            lse = ldg[zz * NX + xx, h : h + 1, :]
            delta = ldg[zz * NX + xx, 2 + h : 3 + h, :]
            nt = (((1,), (1,)), ((), ()))
            scores = lax.dot_general(kb[:, cols], qh, nt, preferred_element_type=jnp.float32)
            dprobs = lax.dot_general(vb[:, cols], gh, nt, preferred_element_type=jnp.float32)
            probs = jnp.where(live, jnp.exp2(scores * (SCALE * LOG2E) - lse), 0.0)
            dscores = (probs * (dprobs - delta)).astype(jnp.bfloat16)
            pall[h, :, at] = probs.astype(jnp.bfloat16)
            sall[h, :, at] = dscores
            dqt = jnp.dot(kt[h], dscores, preferred_element_type=jnp.float32)
            parts.append(dqt.T)
        return parts

    def own_group(zz):
        parts = adjoint(zz, x)
        for h in range(2):
            dqo[zz, :, h * DH : (h + 1) * DH] = parts[h]

    def r1_copy(zz, i):
        n = zz * (NX - 1) + i
        return remote(dqs.at[n], rs1.at[n], s_r1.at[n], r_r1.at[n], dev(z, xpeer(i), y))

    def other_groups(zz, first, last):
        def body(i, c):
            xx = xpeer(i)

            if zz is z and first == 2:
                def arrive(k, c2):
                    wait_far(ypeer(k))
                    return c2
                lax.fori_loop(0, NY - 1, arrive, 0)
            else:
                wait_row(zz, xx)
            wait_lg(zz * NX + xx)
            parts = adjoint(zz, xx)
            n = zz * (NX - 1) + i
            for h in range(2):
                dqs[n, :, :, h * DH : (h + 1) * DH] = parts[h].astype(jnp.bfloat16).reshape(NY, ROWS, DH)
            r1_copy(zz, i).start()
            return c
        lax.fori_loop(first, last, body, 0)

    def r2_copy(zz, yy):
        n = zz * NY + yy
        n_to = jnp.where(zz == z, y, NY)
        return remote(redb.at[n], rs2.at[own], s_r2.at[zz], r_r2.at[n_to], dev(zz, x, yy))

    def reduce_x(zz):
        for i in range(NX - 1):
            r1_copy(zz, i).wait_recv()
        total = dqo[zz]
        for i in range(NX - 1):
            total = total + rs1[zz * (NX - 1) + i].reshape(BLK, COL).astype(jnp.float32)
        redb[pl.ds(zz * NY, NY)] = total.astype(jnp.bfloat16).reshape(NY, ROWS, COL)

    rows_in(z, 2, 0, 4)
    wait_q(zo, y)
    spread_y(zo, 0)
    wait_l(zo * NY + y)
    spread_y(zo, 1)
    spread_x(zo, y, 3)
    spread_far()
    rows_in(z, 2, 4, NY - 1)
    rows_done(z)
    own_group(z)
    rows_in(zo, 3, 0, NY - 1)
    rows_done(zo)
    other_groups(z, 0, 2)
    other_groups(z, 2, 3)
    own_group(zo)
    other_groups(zo, 2, 3)
    other_groups(zo, 0, 2)
    reduce_x(z)

    def near(i, c):
        r2_copy(z, ypeer(i)).start()
        return c
    lax.fori_loop(0, NY - 1, near, 0)
    rs2[own] = redb[own]
    reduce_x(zo)

    def far(i, c):
        r2_copy(zo, (y + i) % NY).start()
        return c
    lax.fori_loop(0, NY, far, 0)

    for h in range(2):
        cols = slice(h * DH, (h + 1) * DH)
        all_q = qg[:, :, h * DH : (h + 1) * DH].reshape(NZ * NX * BLK, DH)
        all_g = qg[:, :, COL + h * DH : COL + (h + 1) * DH].reshape(NZ * NX * BLK, DH)
        key_sum = jnp.dot(sall[h], all_q, preferred_element_type=jnp.float32)
        kob[:, cols] = (key_sum * SCALE).astype(jnp.bfloat16)
        vob[:, cols] = jnp.dot(pall[h], all_g, preferred_element_type=jnp.float32).astype(jnp.bfloat16)

    z_copy(0).wait_send()
    z_copy(1).wait_send()
    blocks = qg.at[pl.ds(0, NY - 1)]
    rows = ldb.at[pl.ds(0, NY - 1)]
    far_copy().wait_send()
    remote(blocks, blocks, s_f.at[1], r_q.at[0], dev(zo, x, y)).wait_send()
    row_copy(zo, 2).wait_send()
    for zz in (z, zo):
        remote(blocks, blocks, s_y.at[zz], r_q.at[0], dev(zo, x, y)).wait_send()
        remote(rows, rows, s_yl.at[zz], r_l.at[0], dev(zo, x, y)).wait_send()
        row_copy(zz, 0).wait_send()
        row_copy(zz, 1).wait_send()
        for i in range(NX - 1):
            xl_copy(zz, i).wait_send()
            r1_copy(zz, i).wait_send()

    def landed_near(i, c):
        l = z * NY + ypeer(i)
        remote(rs2.at[l], rs2.at[l], s_z.at[0], r_r2.at[ypeer(i)], dev(z, x, ypeer(i))).wait_recv()
        return c
    lax.fori_loop(0, NY - 1, landed_near, 0)
    far_part = rs2.at[pl.ds(zo * NY, NY)]
    remote(far_part, far_part, s_z.at[0], r_r2.at[NY], dev(zo, x, y)).wait_recv()

    query_half = (jnp.sum(rs2[...].astype(jnp.float32), axis=0) * SCALE).astype(jnp.bfloat16)
    qg_out[...] = query_half

    def g_copy(j):
        return remote(gs.at[j], gr.at[head], s_g.at[0], r_g.at[head], (obs, j))

    parts = lax.dot_general(query_half, wb[...], (((1,), (1,)), ((), ())), preferred_element_type=jnp.float32)
    for j in range(HEADS):
        gs[j] = parts[:, j * COL : (j + 1) * COL].astype(jnp.bfloat16)

    def grid_send(i, c):
        g_copy((head + 1 + i) % HEADS).start()
        return c
    lax.fori_loop(0, HEADS - 1, grid_send, 0)
    gr[head] = gs[head]

    near_part = redb.at[pl.ds(0, NY - 1)]
    far_sent = redb.at[pl.ds(0, NY)]
    remote(near_part, near_part, s_r2.at[z], r_r2.at[0], dev(zo, x, y)).wait_send()
    remote(far_sent, far_sent, s_r2.at[zo], r_r2.at[0], dev(zo, x, y)).wait_send()

    def grid_landed(i, c):
        j = (head + 1 + i) % HEADS
        remote(gr.at[j], gr.at[j], s_g.at[0], r_g.at[j], (obs, j)).wait_recv()
        return c
    lax.fori_loop(0, HEADS - 1, grid_landed, 0)
    gg_out[...] = jnp.sum(gr[...].astype(jnp.float32), axis=0).astype(jnp.bfloat16)

    pieces = gs.at[pl.ds(0, HEADS - 1)]
    remote(pieces, pieces, s_g.at[0], r_g.at[0], (obs, head)).wait_send()


def finish(kob, vob, qgo, ggo, kg_hbm, vg_hbm, qg_hbm, gg_hbm, sem):
    pairs = ((qgo, qg_hbm), (ggo, gg_hbm), (kob, kg_hbm), (vob, vg_hbm))
    copies = [pltpu.make_async_copy(a, b, sem.at[i]) for i, (a, b) in enumerate(pairs)]
    for c in copies:
        c.start()
    for c in copies:
        c.wait()


def on_device(queries, out_grad, attn_out, logsumexp, keys, values, obs_counts, query_weight):
    bf, f32 = jnp.bfloat16, jnp.float32
    anywhere = pl.BlockSpec(memory_space=pl.ANY)
    vmem = pl.BlockSpec(memory_space=pltpu.VMEM)
    dma = pltpu.SemaphoreType.DMA
    blocks = NZ * NX * NY
    shapes = ((TOK, COL), (TOK, COL), (ROWS, COL), (ROWS, COL))
    held = pl.pallas_call(
        kernel,
        name="adjoint",
        out_shape=tuple(pltpu.VMEM(shape, bf) for shape in shapes),
        in_specs=[anywhere] * 6 + [pl.BlockSpec(memory_space=pltpu.SMEM), anywhere],
        out_specs=(vmem,) * 4,
        scratch_shapes=[
            pltpu.VMEM((blocks, ROWS, 2 * COL), bf),
            pltpu.VMEM((ROWS, COL), bf),
            pltpu.VMEM((2, ROWS), f32),
            pltpu.VMEM((TOK, COL), bf),
            pltpu.VMEM((TOK, COL), bf),
            pltpu.VMEM((2, DH, TOK), bf),
            pltpu.VMEM((HEADS * COL, COL), bf),
            pltpu.VMEM((NZ * NY, 4, BLK), f32),
            pltpu.VMEM((NZ * NX, 4, BLK), f32),
            pltpu.VMEM((2, TOK, NZ * NX * BLK), bf),
            pltpu.VMEM((2, TOK, NZ * NX * BLK), bf),
            pltpu.VMEM((NZ * (NX - 1), NY, ROWS, COL), bf),
            pltpu.VMEM((NZ, BLK, COL), f32),
            pltpu.VMEM((NZ * (NX - 1), NY, ROWS, COL), bf),
            pltpu.VMEM((NZ * NY, ROWS, COL), bf),
            pltpu.VMEM((NZ * NY, ROWS, COL), bf),
            pltpu.VMEM((HEADS, ROWS, COL), bf),
            pltpu.VMEM((HEADS, ROWS, COL), bf),
            dma((7,)), dma((2,)), dma((NZ,)), dma((NZ,)), dma((NZ * (NX - 1),)), dma((2,)), dma((NZ * (NX - 1),)),
            dma((NZ * (NX - 1),)), dma((NZ,)), dma((1,)),
            dma((NZ * NY,)), dma((NZ * NX,)), dma((NY,)), dma((NZ * NY,)), dma((NZ * NX,)), dma((NZ * (NX - 1),)),
            dma((NY + 1,)), dma((HEADS,)),
        ],
        compiler_params=pltpu.CompilerParams(collective_id=0, has_side_effects=True),
    )(queries, out_grad, attn_out, logsumexp.T, keys, values, obs_counts, query_weight)
    return pl.pallas_call(
        finish,
        name="finish",
        out_shape=tuple(jax.ShapeDtypeStruct(shape, bf) for shape in shapes),
        in_specs=[vmem] * 4,
        out_specs=(anywhere,) * 4,
        scratch_shapes=[dma((4,))],
    )(*[pltpu.with_memory_space_constraint(a, pltpu.VMEM) for a in held])


def solution(mesh):
    in_specs = (
        P("obs", "head"),
        P("obs", "head"),
        P("obs", "head"),
        P("obs", "head"),
        P("obs", "head"),
        P("obs", "head"),
        P("obs"),
        P(None, "head"),
    )
    out_specs = (P("obs", "head"), P("obs", "head"), P("obs", "head"), P("obs", "head"))
    return jax.shard_map(
        on_device, mesh=mesh, in_specs=in_specs, out_specs=out_specs, check_vma=False
    )
```

```python
import math

import jax
import jax.numpy as jnp
from jax import lax
from jax.experimental import pallas as pl
from jax.experimental.pallas import tpu as pltpu
from jax.sharding import PartitionSpec as P

MESH = pl.DeviceIdType.MESH
DH = 128
NZ, NX, NY = 2, 4, 8
HEADS = 8
ROWS = 16
TOK = 384
COL = 256
BLK = NY * ROWS
SCALE = 1.0 / math.sqrt(DH)
LOG2E = math.log2(math.e)


def ring_offset(i, n):
    d = i // 2 + 1
    odd = i % 2
    return (1 - odd) * d + odd * (n - d)


def kernel(
    q_hbm, g_hbm, o_hbm, lse_hbm, k_hbm, v_hbm, cnt, w_hbm,
    kob, vob, qg_out, gg_out,
    qg, att, lse_v, kb, vb, kt, wb,
    ldb, ldg, pall, sall, dqs, dqo, rs1, redb, rs2, gs, gr,
    sem_in, s_z, s_y, s_yl, s_x, s_f, s_xl, s_r1, s_r2, s_g,
    r_q, r_x, r_f, r_l, r_lg, r_r1, r_r2, r_g,
):
    obs = lax.axis_index("obs")
    head = lax.axis_index("head")
    z = obs // (NX * NY)
    x = (obs // NY) % NX
    y = obs % NY
    zo = 1 - z

    def dev(zz, xx, yy):
        return ((zz * NX + xx) * NY + yy, head)

    def slot(zz, xx, yy):
        return (zz * NX + xx) * NY + yy

    def xpeer(i):
        return (x + ring_offset(i, NX)) % NX

    def xsource(i):
        return (x + NX - ring_offset(i, NX)) % NX

    def ypeer(i):
        return (y + ring_offset(i, NY)) % NY

    def remote(src, dst, ssem, rsem, device):
        return pltpu.make_async_remote_copy(
            src_ref=src, dst_ref=dst, send_sem=ssem, recv_sem=rsem,
            device_id=device, device_id_type=MESH)

    me = slot(z, x, y)
    loads = [
        pltpu.make_async_copy(q_hbm, qg.at[me, :, pl.ds(0, COL)], sem_in.at[0]),
        pltpu.make_async_copy(g_hbm, qg.at[me, :, pl.ds(COL, COL)], sem_in.at[1]),
        pltpu.make_async_copy(o_hbm, att, sem_in.at[2]),
        pltpu.make_async_copy(lse_hbm, lse_v, sem_in.at[3]),
        pltpu.make_async_copy(k_hbm, kb, sem_in.at[4]),
        pltpu.make_async_copy(v_hbm, vb, sem_in.at[5]),
        pltpu.make_async_copy(w_hbm, wb, sem_in.at[6]),
    ]
    for c in loads:
        c.start()

    barrier = pltpu.get_barrier_semaphore()

    def hello(device):
        pl.semaphore_signal(barrier, inc=1, device_id=device, device_id_type=MESH)

    hello(dev(zo, x, y))

    def hello_y(i, c):
        hello(dev(z, x, ypeer(i)))
        return c

    lax.fori_loop(0, NY - 1, hello_y, 0)

    def hello_x(i, c):
        hello(dev(z, xpeer(i), y))
        return c

    lax.fori_loop(0, NX - 1, hello_x, 0)

    def hello_h(i, c):
        hello((obs, (head + 1 + i) % HEADS))
        return c

    lax.fori_loop(0, HEADS - 1, hello_h, 0)

    for c in loads[:2]:
        c.wait()
    own = z * NY + y
    pl.semaphore_wait(barrier, 1 + NY - 1 + NX - 1 + HEADS - 1)

    def z_copy(k):
        if k == 0:
            return remote(qg.at[me], qg.at[me], s_z.at[0], r_q.at[z * NY + y], dev(zo, x, y))
        return remote(ldb.at[own], ldb.at[own], s_z.at[1], r_l.at[own], dev(zo, x, y))

    def y_copies(zz, i):
        s = slot(zz, x, y)
        l = zz * NY + y
        to = dev(z, x, ypeer(i))
        return (remote(qg.at[s], qg.at[s], s_y.at[zz], r_q.at[l], to),
                remote(ldb.at[l], ldb.at[l], s_yl.at[zz], r_l.at[l], to))

    def strip(zz, xx):
        return qg.at[pl.ds(slot(zz, xx, 0), NY)]

    def row_copy(zz, i):
        return remote(strip(zz, x), strip(zz, x), s_x.at[zz * (NX - 1) + i], r_x.at[zz * NX + x], dev(z, xpeer(i), y))

    def x_copy(zz, yy, i):
        s = slot(zz, x, yy)
        return remote(qg.at[s], qg.at[s], s_x.at[zz * (NX - 1) + i], r_x.at[zz * NX + x], dev(z, xpeer(i), y))

    def xl_copy(zz, i):
        n = zz * NX + x
        return remote(ldg.at[n], ldg.at[n], s_xl.at[zz * (NX - 1) + i], r_lg.at[n], dev(z, xpeer(i), y))

    def wait_q(zz, yy):
        s = slot(zz, x, yy)
        remote(qg.at[s], qg.at[s], s_z.at[0], r_q.at[zz * NY + yy], dev(zo, x, y)).wait_recv()

    def wait_row(zz, xx):
        remote(strip(zz, xx), strip(zz, xx), s_x.at[0], r_x.at[zz * NX + xx], dev(z, xx, y)).wait_recv()

    def wait_l(l):
        remote(ldb.at[l], ldb.at[l], s_z.at[1], r_l.at[l], dev(zo, x, y)).wait_recv()

    def wait_lg(n):
        remote(ldg.at[n], ldg.at[n], s_z.at[1], r_lg.at[n], dev(zo, x, y)).wait_recv()

    def spread_y(zz, which):
        def body(i, c):
            y_copies(zz, i)[which].start()
            return c
        lax.fori_loop(0, NY - 1, body, 0)

    def spread_x(zz, yy, sides):
        def body(i, c):
            x_copy(zz, yy, i).start()
            return c
        lax.fori_loop(0, sides, body, 0)

    xf = (x + NX // 2) % NX

    def far_copy():
        return remote(qg.at[me], qg.at[me], s_f.at[0], r_f.at[y], dev(z, xf, y))

    def far_y_copy(i):
        s = slot(z, xf, y)
        return remote(qg.at[s], qg.at[s], s_f.at[1], r_f.at[y], dev(z, x, ypeer(i)))

    def wait_far(yy):
        s = slot(z, xf, yy)
        remote(qg.at[s], qg.at[s], s_f.at[0], r_f.at[yy], dev(z, xf, y)).wait_recv()

    def spread_far():
        wait_far(y)

        def body(i, c):
            far_y_copy(i).start()
            return c
        lax.fori_loop(0, NY - 1, body, 0)

    def rows_in(zz, sides, first, last):
        def body(i, c):
            yy = ypeer(i)
            wait_q(zz, yy)
            spread_x(zz, yy, sides)
            return c
        lax.fori_loop(first, last, body, 0)

    def rows_done(zz):
        def body_l(i, c):
            wait_l(zz * NY + ypeer(i))
            return c
        lax.fori_loop(0, NY - 1, body_l, 0)
        total = ldb[zz * NY]
        for k in range(1, NY):
            total = total + ldb[zz * NY + k]
        ldg[zz * NX + x] = total

        def body_g(i, c):
            xl_copy(zz, i).start()
            return c
        lax.fori_loop(0, NX - 1, body_g, 0)

    z_copy(0).start()
    spread_y(z, 0)
    far_copy().start()
    spread_x(z, y, 2)

    for c in loads[2:4]:
        c.wait()

    row = lax.broadcasted_iota(jnp.int32, (ROWS, BLK), 0)
    lane = lax.broadcasted_iota(jnp.int32, (ROWS, BLK), 1)
    mine = lane == row + y * ROWS
    my_lanes = lax.broadcasted_iota(jnp.int32, (1, BLK), 1) // ROWS == y
    for h in range(2):
        og = qg[me, :, COL + h * DH : COL + (h + 1) * DH].astype(jnp.float32)
        ao = att[:, h * DH : (h + 1) * DH].astype(jnp.float32)
        delta = jnp.sum(og * ao, axis=1, keepdims=True)
        lse = jnp.concatenate([lse_v[h : h + 1, :] * LOG2E] * NY, axis=1)
        ldb[own, h : h + 1, :] = jnp.where(my_lanes, lse, 0.0)
        ldb[own, 2 + h : 3 + h, :] = jnp.sum(jnp.where(mine, delta, 0.0), axis=0, keepdims=True)

    z_copy(1).start()
    spread_y(z, 1)

    for c in loads[4:]:
        c.wait()
    for h in range(2):
        kt[h] = kb[:, h * DH : (h + 1) * DH].astype(jnp.float32).T.astype(jnp.bfloat16)
    live = lax.broadcasted_iota(jnp.int32, (TOK, BLK), 0) < cnt[0]

    def adjoint(zz, xx):
        base = slot(zz, xx, 0)
        at = pl.ds(pl.multiple_of(base * ROWS, BLK), BLK)
        parts = []
        for h in range(2):
            cols = slice(h * DH, (h + 1) * DH)
            qh = qg[pl.ds(base, NY), :, h * DH : (h + 1) * DH].reshape(BLK, DH)
            gh = qg[pl.ds(base, NY), :, COL + h * DH : COL + (h + 1) * DH].reshape(BLK, DH)
            lse = ldg[zz * NX + xx, h : h + 1, :]
            delta = ldg[zz * NX + xx, 2 + h : 3 + h, :]
            nt = (((1,), (1,)), ((), ()))
            scores = lax.dot_general(kb[:, cols], qh, nt, preferred_element_type=jnp.float32)
            dprobs = lax.dot_general(vb[:, cols], gh, nt, preferred_element_type=jnp.float32)
            probs = jnp.where(live, jnp.exp2(scores * (SCALE * LOG2E) - lse), 0.0)
            dscores = (probs * (dprobs - delta)).astype(jnp.bfloat16)
            pall[h, :, at] = probs.astype(jnp.bfloat16)
            sall[h, :, at] = dscores
            dqt = jnp.dot(kt[h], dscores, preferred_element_type=jnp.float32)
            parts.append(dqt.T)
        return parts

    def own_group(zz):
        parts = adjoint(zz, x)
        for h in range(2):
            dqo[zz, :, h * DH : (h + 1) * DH] = parts[h]

    def r1_copy(zz, i):
        n = zz * (NX - 1) + i
        return remote(dqs.at[n], rs1.at[n], s_r1.at[n], r_r1.at[n], dev(z, xpeer(i), y))

    def other_groups(zz, first, last):
        def body(i, c):
            xx = xpeer(i)

            if zz is z and first == 2:
                def arrive(k, c2):
                    wait_far(ypeer(k))
                    return c2
                lax.fori_loop(0, NY - 1, arrive, 0)
            else:
                wait_row(zz, xx)
            wait_lg(zz * NX + xx)
            parts = adjoint(zz, xx)
            n = zz * (NX - 1) + i
            for h in range(2):
                dqs[n, :, :, h * DH : (h + 1) * DH] = parts[h].astype(jnp.bfloat16).reshape(NY, ROWS, DH)
            r1_copy(zz, i).start()
            return c
        lax.fori_loop(first, last, body, 0)

    def r2_copy(zz, yy):
        n = zz * NY + yy
        n_to = jnp.where(zz == z, y, NY)
        return remote(redb.at[n], rs2.at[own], s_r2.at[zz], r_r2.at[n_to], dev(zz, x, yy))

    def reduce_x(zz):
        for i in range(NX - 1):
            r1_copy(zz, i).wait_recv()
        total = dqo[zz]
        for i in range(NX - 1):
            total = total + rs1[zz * (NX - 1) + i].reshape(BLK, COL).astype(jnp.float32)
        redb[pl.ds(zz * NY, NY)] = total.astype(jnp.bfloat16).reshape(NY, ROWS, COL)

    rows_in(z, 2, 0, 4)
    wait_q(zo, y)
    spread_y(zo, 0)
    wait_l(zo * NY + y)
    spread_y(zo, 1)
    spread_x(zo, y, 3)
    spread_far()
    rows_in(z, 2, 4, NY - 1)
    rows_done(z)
    own_group(z)
    rows_in(zo, 3, 0, NY - 1)
    rows_done(zo)
    own_group(zo)
    other_groups(z, 0, 2)
    other_groups(z, 2, 3)
    other_groups(zo, 0, 2)
    other_groups(zo, 2, 3)
    reduce_x(z)

    def near(i, c):
        r2_copy(z, ypeer(i)).start()
        return c
    lax.fori_loop(0, NY - 1, near, 0)
    rs2[own] = redb[own]
    reduce_x(zo)

    def far(i, c):
        off = jnp.where(i == 0, NY // 2, NY // 2 + ring_offset(i - 1, NY))
        r2_copy(zo, (y + off) % NY).start()
        return c
    lax.fori_loop(0, NY, far, 0)

    for h in range(2):
        cols = slice(h * DH, (h + 1) * DH)
        all_q = qg[:, :, h * DH : (h + 1) * DH].reshape(NZ * NX * BLK, DH)
        all_g = qg[:, :, COL + h * DH : COL + (h + 1) * DH].reshape(NZ * NX * BLK, DH)
        key_sum = jnp.dot(sall[h], all_q, preferred_element_type=jnp.float32)
        kob[:, cols] = (key_sum * SCALE).astype(jnp.bfloat16)
        vob[:, cols] = jnp.dot(pall[h], all_g, preferred_element_type=jnp.float32).astype(jnp.bfloat16)

    z_copy(0).wait_send()
    z_copy(1).wait_send()
    blocks = qg.at[pl.ds(0, NY - 1)]
    rows = ldb.at[pl.ds(0, NY - 1)]
    far_copy().wait_send()
    remote(blocks, blocks, s_f.at[1], r_q.at[0], dev(zo, x, y)).wait_send()
    row_copy(zo, 2).wait_send()
    for zz in (z, zo):
        remote(blocks, blocks, s_y.at[zz], r_q.at[0], dev(zo, x, y)).wait_send()
        remote(rows, rows, s_yl.at[zz], r_l.at[0], dev(zo, x, y)).wait_send()
        row_copy(zz, 0).wait_send()
        row_copy(zz, 1).wait_send()
        for i in range(NX - 1):
            xl_copy(zz, i).wait_send()
            r1_copy(zz, i).wait_send()

    def landed_near(i, c):
        l = z * NY + ypeer(i)
        remote(rs2.at[l], rs2.at[l], s_z.at[0], r_r2.at[ypeer(i)], dev(z, x, ypeer(i))).wait_recv()
        return c
    lax.fori_loop(0, NY - 1, landed_near, 0)
    far_part = rs2.at[pl.ds(zo * NY, NY)]
    remote(far_part, far_part, s_z.at[0], r_r2.at[NY], dev(zo, x, y)).wait_recv()

    query_half = (jnp.sum(rs2[...].astype(jnp.float32), axis=0) * SCALE).astype(jnp.bfloat16)
    qg_out[...] = query_half

    def g_copy(j):
        return remote(gs.at[j], gr.at[head], s_g.at[0], r_g.at[head], (obs, j))

    parts = lax.dot_general(query_half, wb[...], (((1,), (1,)), ((), ())), preferred_element_type=jnp.float32)
    for j in range(HEADS):
        gs[j] = parts[:, j * COL : (j + 1) * COL].astype(jnp.bfloat16)

    def grid_send(i, c):
        g_copy((head + 1 + i) % HEADS).start()
        return c
    lax.fori_loop(0, HEADS - 1, grid_send, 0)
    gr[head] = gs[head]

    near_part = redb.at[pl.ds(0, NY - 1)]
    far_sent = redb.at[pl.ds(0, NY)]
    remote(near_part, near_part, s_r2.at[z], r_r2.at[0], dev(zo, x, y)).wait_send()
    remote(far_sent, far_sent, s_r2.at[zo], r_r2.at[0], dev(zo, x, y)).wait_send()

    def grid_landed(i, c):
        j = (head + 1 + i) % HEADS
        remote(gr.at[j], gr.at[j], s_g.at[0], r_g.at[j], (obs, j)).wait_recv()
        return c
    lax.fori_loop(0, HEADS - 1, grid_landed, 0)
    gg_out[...] = jnp.sum(gr[...].astype(jnp.float32), axis=0).astype(jnp.bfloat16)

    pieces = gs.at[pl.ds(0, HEADS - 1)]
    remote(pieces, pieces, s_g.at[0], r_g.at[0], (obs, head)).wait_send()


def finish(kob, vob, qgo, ggo, kg_hbm, vg_hbm, qg_hbm, gg_hbm, sem):
    pairs = ((qgo, qg_hbm), (ggo, gg_hbm), (kob, kg_hbm), (vob, vg_hbm))
    copies = [pltpu.make_async_copy(a, b, sem.at[i]) for i, (a, b) in enumerate(pairs)]
    for c in copies:
        c.start()
    for c in copies:
        c.wait()


def on_device(queries, out_grad, attn_out, logsumexp, keys, values, obs_counts, query_weight):
    bf, f32 = jnp.bfloat16, jnp.float32
    anywhere = pl.BlockSpec(memory_space=pl.ANY)
    vmem = pl.BlockSpec(memory_space=pltpu.VMEM)
    dma = pltpu.SemaphoreType.DMA
    blocks = NZ * NX * NY
    shapes = ((TOK, COL), (TOK, COL), (ROWS, COL), (ROWS, COL))
    held = pl.pallas_call(
        kernel,
        name="adjoint",
        out_shape=tuple(pltpu.VMEM(shape, bf) for shape in shapes),
        in_specs=[anywhere] * 6 + [pl.BlockSpec(memory_space=pltpu.SMEM), anywhere],
        out_specs=(vmem,) * 4,
        scratch_shapes=[
            pltpu.VMEM((blocks, ROWS, 2 * COL), bf),
            pltpu.VMEM((ROWS, COL), bf),
            pltpu.VMEM((2, ROWS), f32),
            pltpu.VMEM((TOK, COL), bf),
            pltpu.VMEM((TOK, COL), bf),
            pltpu.VMEM((2, DH, TOK), bf),
            pltpu.VMEM((HEADS * COL, COL), bf),
            pltpu.VMEM((NZ * NY, 4, BLK), f32),
            pltpu.VMEM((NZ * NX, 4, BLK), f32),
            pltpu.VMEM((2, TOK, NZ * NX * BLK), bf),
            pltpu.VMEM((2, TOK, NZ * NX * BLK), bf),
            pltpu.VMEM((NZ * (NX - 1), NY, ROWS, COL), bf),
            pltpu.VMEM((NZ, BLK, COL), f32),
            pltpu.VMEM((NZ * (NX - 1), NY, ROWS, COL), bf),
            pltpu.VMEM((NZ * NY, ROWS, COL), bf),
            pltpu.VMEM((NZ * NY, ROWS, COL), bf),
            pltpu.VMEM((HEADS, ROWS, COL), bf),
            pltpu.VMEM((HEADS, ROWS, COL), bf),
            dma((7,)), dma((2,)), dma((NZ,)), dma((NZ,)), dma((NZ * (NX - 1),)), dma((2,)), dma((NZ * (NX - 1),)),
            dma((NZ * (NX - 1),)), dma((NZ,)), dma((1,)),
            dma((NZ * NY,)), dma((NZ * NX,)), dma((NY,)), dma((NZ * NY,)), dma((NZ * NX,)), dma((NZ * (NX - 1),)),
            dma((NY + 1,)), dma((HEADS,)),
        ],
        compiler_params=pltpu.CompilerParams(collective_id=0, has_side_effects=True),
    )(queries, out_grad, attn_out, logsumexp.T, keys, values, obs_counts, query_weight)
    return pl.pallas_call(
        finish,
        name="finish",
        out_shape=tuple(jax.ShapeDtypeStruct(shape, bf) for shape in shapes),
        in_specs=[vmem] * 4,
        out_specs=(anywhere,) * 4,
        scratch_shapes=[dma((4,))],
    )(*[pltpu.with_memory_space_constraint(a, pltpu.VMEM) for a in held])


def solution(mesh):
    in_specs = (
        P("obs", "head"),
        P("obs", "head"),
        P("obs", "head"),
        P("obs", "head"),
        P("obs", "head"),
        P("obs", "head"),
        P("obs"),
        P(None, "head"),
    )
    out_specs = (P("obs", "head"), P("obs", "head"), P("obs", "head"), P("obs", "head"))
    return jax.shard_map(
        on_device, mesh=mesh, in_specs=in_specs, out_specs=out_specs, check_vma=False
    )
```

```python
import math

import jax
import jax.numpy as jnp
from jax import lax
from jax.experimental import pallas as pl
from jax.experimental.pallas import tpu as pltpu
from jax.sharding import PartitionSpec as P

MESH = pl.DeviceIdType.MESH
DH = 128
NZ, NX, NY = 2, 4, 8
HEADS = 8
ROWS = 16
TOK = 384
COL = 256
BLK = NY * ROWS
SCALE = 1.0 / math.sqrt(DH)
LOG2E = math.log2(math.e)


def ring_offset(i, n):
    d = i // 2 + 1
    odd = i % 2
    return (1 - odd) * d + odd * (n - d)


def kernel(
    q_hbm, g_hbm, o_hbm, lse_hbm, k_hbm, v_hbm, cnt, w_hbm,
    kob, vob, qg_out, gg_out,
    qg, att, lse_v, kb, vb, kt, wb,
    ldb, ldg, pall, sall, dqs, dqo, rs1, redb, rs2, gs, gr,
    sem_in, s_z, s_y, s_yl, s_x, s_f, s_xl, s_r1, s_r2, s_g,
    r_q, r_x, r_f, r_l, r_lg, r_r1, r_r2, r_g,
):
    obs = lax.axis_index("obs")
    head = lax.axis_index("head")
    z = obs // (NX * NY)
    x = (obs // NY) % NX
    y = obs % NY
    zo = 1 - z

    def dev(zz, xx, yy):
        return ((zz * NX + xx) * NY + yy, head)

    def slot(zz, xx, yy):
        return (zz * NX + xx) * NY + yy

    def xpeer(i):
        return (x + ring_offset(i, NX)) % NX

    def xsource(i):
        return (x + NX - ring_offset(i, NX)) % NX

    def ypeer(i):
        return (y + ring_offset(i, NY)) % NY

    def remote(src, dst, ssem, rsem, device):
        return pltpu.make_async_remote_copy(
            src_ref=src, dst_ref=dst, send_sem=ssem, recv_sem=rsem,
            device_id=device, device_id_type=MESH)

    me = slot(z, x, y)
    loads = [
        pltpu.make_async_copy(q_hbm, qg.at[me, :, pl.ds(0, COL)], sem_in.at[0]),
        pltpu.make_async_copy(g_hbm, qg.at[me, :, pl.ds(COL, COL)], sem_in.at[1]),
        pltpu.make_async_copy(o_hbm, att, sem_in.at[2]),
        pltpu.make_async_copy(lse_hbm, lse_v, sem_in.at[3]),
        pltpu.make_async_copy(k_hbm, kb, sem_in.at[4]),
        pltpu.make_async_copy(v_hbm, vb, sem_in.at[5]),
        pltpu.make_async_copy(w_hbm, wb, sem_in.at[6]),
    ]
    for c in loads:
        c.start()

    barrier = pltpu.get_barrier_semaphore()

    def hello(device):
        pl.semaphore_signal(barrier, inc=1, device_id=device, device_id_type=MESH)

    hello(dev(zo, x, y))

    def hello_y(i, c):
        hello(dev(z, x, ypeer(i)))
        return c

    lax.fori_loop(0, NY - 1, hello_y, 0)

    def hello_x(i, c):
        hello(dev(z, xpeer(i), y))
        return c

    lax.fori_loop(0, NX - 1, hello_x, 0)

    def hello_h(i, c):
        hello((obs, (head + 1 + i) % HEADS))
        return c

    lax.fori_loop(0, HEADS - 1, hello_h, 0)

    for c in loads[:2]:
        c.wait()
    own = z * NY + y
    pl.semaphore_wait(barrier, 1 + NY - 1 + NX - 1 + HEADS - 1)

    def z_copy(k):
        if k == 0:
            return remote(qg.at[me], qg.at[me], s_z.at[0], r_q.at[z * NY + y], dev(zo, x, y))
        return remote(ldb.at[own], ldb.at[own], s_z.at[1], r_l.at[own], dev(zo, x, y))

    def y_copies(zz, i):
        s = slot(zz, x, y)
        l = zz * NY + y
        to = dev(z, x, ypeer(i))
        return (remote(qg.at[s], qg.at[s], s_y.at[zz], r_q.at[l], to),
                remote(ldb.at[l], ldb.at[l], s_yl.at[zz], r_l.at[l], to))

    def strip(zz, xx):
        return qg.at[pl.ds(slot(zz, xx, 0), NY)]

    def row_copy(zz, i):
        return remote(strip(zz, x), strip(zz, x), s_x.at[zz * (NX - 1) + i], r_x.at[zz * NX + x], dev(z, xpeer(i), y))

    def x_copy(zz, yy, i):
        s = slot(zz, x, yy)
        return remote(qg.at[s], qg.at[s], s_x.at[zz * (NX - 1) + i], r_x.at[zz * NX + x], dev(z, xpeer(i), y))

    def xl_copy(zz, i):
        n = zz * NX + x
        return remote(ldg.at[n], ldg.at[n], s_xl.at[zz * (NX - 1) + i], r_lg.at[n], dev(z, xpeer(i), y))

    def wait_q(zz, yy):
        s = slot(zz, x, yy)
        remote(qg.at[s], qg.at[s], s_z.at[0], r_q.at[zz * NY + yy], dev(zo, x, y)).wait_recv()

    def wait_row(zz, xx):
        remote(strip(zz, xx), strip(zz, xx), s_x.at[0], r_x.at[zz * NX + xx], dev(z, xx, y)).wait_recv()

    def wait_l(l):
        remote(ldb.at[l], ldb.at[l], s_z.at[1], r_l.at[l], dev(zo, x, y)).wait_recv()

    def wait_lg(n):
        remote(ldg.at[n], ldg.at[n], s_z.at[1], r_lg.at[n], dev(zo, x, y)).wait_recv()

    def spread_y(zz, which):
        def body(i, c):
            y_copies(zz, i)[which].start()
            return c
        lax.fori_loop(0, NY - 1, body, 0)

    def spread_x(zz, yy, sides):
        def body(i, c):
            x_copy(zz, yy, i).start()
            return c
        lax.fori_loop(0, sides, body, 0)

    xf = (x + NX // 2) % NX

    def far_copy():
        return remote(qg.at[me], qg.at[me], s_f.at[0], r_f.at[y], dev(z, xf, y))

    def far_y_copy(i):
        s = slot(z, xf, y)
        return remote(qg.at[s], qg.at[s], s_f.at[1], r_f.at[y], dev(z, x, ypeer(i)))

    def wait_far(yy):
        s = slot(z, xf, yy)
        remote(qg.at[s], qg.at[s], s_f.at[0], r_f.at[yy], dev(z, xf, y)).wait_recv()

    def spread_far():
        wait_far(y)

        def body(i, c):
            far_y_copy(i).start()
            return c
        lax.fori_loop(0, NY - 1, body, 0)

    def rows_in(zz, sides, first, last):
        def body(i, c):
            yy = ypeer(i)
            wait_q(zz, yy)
            spread_x(zz, yy, sides)
            return c
        lax.fori_loop(first, last, body, 0)

    def rows_done(zz):
        def body_l(i, c):
            wait_l(zz * NY + ypeer(i))
            return c
        lax.fori_loop(0, NY - 1, body_l, 0)
        total = ldb[zz * NY]
        for k in range(1, NY):
            total = total + ldb[zz * NY + k]
        ldg[zz * NX + x] = total

        def body_g(i, c):
            xl_copy(zz, i).start()
            return c
        lax.fori_loop(0, NX - 1, body_g, 0)

    z_copy(0).start()
    spread_y(z, 0)
    far_copy().start()
    spread_x(z, y, 2)

    for c in loads[2:4]:
        c.wait()

    row = lax.broadcasted_iota(jnp.int32, (ROWS, BLK), 0)
    lane = lax.broadcasted_iota(jnp.int32, (ROWS, BLK), 1)
    mine = lane == row + y * ROWS
    my_lanes = lax.broadcasted_iota(jnp.int32, (1, BLK), 1) // ROWS == y
    for h in range(2):
        og = qg[me, :, COL + h * DH : COL + (h + 1) * DH].astype(jnp.float32)
        ao = att[:, h * DH : (h + 1) * DH].astype(jnp.float32)
        delta = jnp.sum(og * ao, axis=1, keepdims=True)
        lse = jnp.concatenate([lse_v[h : h + 1, :] * LOG2E] * NY, axis=1)
        ldb[own, h : h + 1, :] = jnp.where(my_lanes, lse, 0.0)
        ldb[own, 2 + h : 3 + h, :] = jnp.sum(jnp.where(mine, delta, 0.0), axis=0, keepdims=True)

    z_copy(1).start()
    spread_y(z, 1)

    for c in loads[4:]:
        c.wait()
    for h in range(2):
        kt[h] = kb[:, h * DH : (h + 1) * DH].astype(jnp.float32).T.astype(jnp.bfloat16)
    live = lax.broadcasted_iota(jnp.int32, (TOK, BLK), 0) < cnt[0]

    def adjoint(zz, xx):
        base = slot(zz, xx, 0)
        at = pl.ds(pl.multiple_of(base * ROWS, BLK), BLK)
        parts = []
        for h in range(2):
            cols = slice(h * DH, (h + 1) * DH)
            qh = qg[pl.ds(base, NY), :, h * DH : (h + 1) * DH].reshape(BLK, DH)
            gh = qg[pl.ds(base, NY), :, COL + h * DH : COL + (h + 1) * DH].reshape(BLK, DH)
            lse = ldg[zz * NX + xx, h : h + 1, :]
            delta = ldg[zz * NX + xx, 2 + h : 3 + h, :]
            nt = (((1,), (1,)), ((), ()))
            scores = lax.dot_general(kb[:, cols], qh, nt, preferred_element_type=jnp.float32)
            dprobs = lax.dot_general(vb[:, cols], gh, nt, preferred_element_type=jnp.float32)
            probs = jnp.where(live, jnp.exp2(scores * (SCALE * LOG2E) - lse), 0.0)
            dscores = (probs * (dprobs - delta)).astype(jnp.bfloat16)
            pall[h, :, at] = probs.astype(jnp.bfloat16)
            sall[h, :, at] = dscores
            dqt = jnp.dot(kt[h], dscores, preferred_element_type=jnp.float32)
            parts.append(dqt.T)
        return parts

    def own_group(zz):
        parts = adjoint(zz, x)
        for h in range(2):
            dqo[zz, :, h * DH : (h + 1) * DH] = parts[h]

    def r1_copy(zz, i):
        n = zz * (NX - 1) + i
        return remote(dqs.at[n], rs1.at[n], s_r1.at[n], r_r1.at[n], dev(z, xpeer(i), y))

    def other_groups(zz, first, last):
        def body(i, c):
            xx = xpeer(i)

            if zz is z and first == 2:
                def arrive(k, c2):
                    wait_far(ypeer(k))
                    return c2
                lax.fori_loop(0, NY - 1, arrive, 0)
            else:
                wait_row(zz, xx)
            wait_lg(zz * NX + xx)
            parts = adjoint(zz, xx)
            n = zz * (NX - 1) + i
            for h in range(2):
                dqs[n, :, :, h * DH : (h + 1) * DH] = parts[h].astype(jnp.bfloat16).reshape(NY, ROWS, DH)
            r1_copy(zz, i).start()
            return c
        lax.fori_loop(first, last, body, 0)

    def r2_copy(zz, yy):
        n = zz * NY + yy
        n_to = jnp.where(zz == z, y, NY)
        return remote(redb.at[n], rs2.at[own], s_r2.at[zz], r_r2.at[n_to], dev(zz, x, yy))

    def reduce_x(zz):
        for i in range(NX - 1):
            r1_copy(zz, i).wait_recv()
        total = dqo[zz]
        for i in range(NX - 1):
            total = total + rs1[zz * (NX - 1) + i].reshape(BLK, COL).astype(jnp.float32)
        redb[pl.ds(zz * NY, NY)] = total.astype(jnp.bfloat16).reshape(NY, ROWS, COL)

    rows_in(z, 2, 0, 4)
    wait_q(zo, y)
    spread_y(zo, 0)
    spread_x(zo, y, 3)
    rows_in(z, 2, 4, NY - 1)
    wait_l(zo * NY + y)
    spread_y(zo, 1)
    spread_far()
    rows_done(z)
    own_group(z)
    rows_in(zo, 3, 0, NY - 1)
    rows_done(zo)
    own_group(zo)
    other_groups(z, 0, 2)
    other_groups(z, 2, 3)
    other_groups(zo, 0, 2)
    other_groups(zo, 2, 3)
    reduce_x(z)

    def near(i, c):
        r2_copy(z, ypeer(i)).start()
        return c
    lax.fori_loop(0, NY - 1, near, 0)
    rs2[own] = redb[own]
    reduce_x(zo)

    def far(i, c):
        off = jnp.where(i == 0, NY // 2, NY // 2 + ring_offset(i - 1, NY))
        r2_copy(zo, (y + off) % NY).start()
        return c
    lax.fori_loop(0, NY, far, 0)

    for h in range(2):
        cols = slice(h * DH, (h + 1) * DH)
        all_q = qg[:, :, h * DH : (h + 1) * DH].reshape(NZ * NX * BLK, DH)
        all_g = qg[:, :, COL + h * DH : COL + (h + 1) * DH].reshape(NZ * NX * BLK, DH)
        key_sum = jnp.dot(sall[h], all_q, preferred_element_type=jnp.float32)
        kob[:, cols] = (key_sum * SCALE).astype(jnp.bfloat16)
        vob[:, cols] = jnp.dot(pall[h], all_g, preferred_element_type=jnp.float32).astype(jnp.bfloat16)

    z_copy(0).wait_send()
    z_copy(1).wait_send()
    blocks = qg.at[pl.ds(0, NY - 1)]
    rows = ldb.at[pl.ds(0, NY - 1)]
    far_copy().wait_send()
    remote(blocks, blocks, s_f.at[1], r_q.at[0], dev(zo, x, y)).wait_send()
    row_copy(zo, 2).wait_send()
    for zz in (z, zo):
        remote(blocks, blocks, s_y.at[zz], r_q.at[0], dev(zo, x, y)).wait_send()
        remote(rows, rows, s_yl.at[zz], r_l.at[0], dev(zo, x, y)).wait_send()
        row_copy(zz, 0).wait_send()
        row_copy(zz, 1).wait_send()
        for i in range(NX - 1):
            xl_copy(zz, i).wait_send()
            r1_copy(zz, i).wait_send()

    def landed_near(i, c):
        l = z * NY + ypeer(i)
        remote(rs2.at[l], rs2.at[l], s_z.at[0], r_r2.at[ypeer(i)], dev(z, x, ypeer(i))).wait_recv()
        return c
    lax.fori_loop(0, NY - 1, landed_near, 0)
    far_part = rs2.at[pl.ds(zo * NY, NY)]
    remote(far_part, far_part, s_z.at[0], r_r2.at[NY], dev(zo, x, y)).wait_recv()

    query_half = (jnp.sum(rs2[...].astype(jnp.float32), axis=0) * SCALE).astype(jnp.bfloat16)
    qg_out[...] = query_half

    def g_copy(j):
        return remote(gs.at[j], gr.at[head], s_g.at[0], r_g.at[head], (obs, j))

    parts = lax.dot_general(query_half, wb[...], (((1,), (1,)), ((), ())), preferred_element_type=jnp.float32)
    for j in range(HEADS):
        gs[j] = parts[:, j * COL : (j + 1) * COL].astype(jnp.bfloat16)

    def grid_send(i, c):
        g_copy((head + 1 + i) % HEADS).start()
        return c
    lax.fori_loop(0, HEADS - 1, grid_send, 0)
    gr[head] = gs[head]

    near_part = redb.at[pl.ds(0, NY - 1)]
    far_sent = redb.at[pl.ds(0, NY)]
    remote(near_part, near_part, s_r2.at[z], r_r2.at[0], dev(zo, x, y)).wait_send()
    remote(far_sent, far_sent, s_r2.at[zo], r_r2.at[0], dev(zo, x, y)).wait_send()

    def grid_landed(i, c):
        j = (head + 1 + i) % HEADS
        remote(gr.at[j], gr.at[j], s_g.at[0], r_g.at[j], (obs, j)).wait_recv()
        return c
    lax.fori_loop(0, HEADS - 1, grid_landed, 0)
    gg_out[...] = jnp.sum(gr[...].astype(jnp.float32), axis=0).astype(jnp.bfloat16)

    pieces = gs.at[pl.ds(0, HEADS - 1)]
    remote(pieces, pieces, s_g.at[0], r_g.at[0], (obs, head)).wait_send()


def finish(kob, vob, qgo, ggo, kg_hbm, vg_hbm, qg_hbm, gg_hbm, sem):
    pairs = ((qgo, qg_hbm), (ggo, gg_hbm), (kob, kg_hbm), (vob, vg_hbm))
    copies = [pltpu.make_async_copy(a, b, sem.at[i]) for i, (a, b) in enumerate(pairs)]
    for c in copies:
        c.start()
    for c in copies:
        c.wait()


def on_device(queries, out_grad, attn_out, logsumexp, keys, values, obs_counts, query_weight):
    bf, f32 = jnp.bfloat16, jnp.float32
    anywhere = pl.BlockSpec(memory_space=pl.ANY)
    vmem = pl.BlockSpec(memory_space=pltpu.VMEM)
    dma = pltpu.SemaphoreType.DMA
    blocks = NZ * NX * NY
    shapes = ((TOK, COL), (TOK, COL), (ROWS, COL), (ROWS, COL))
    held = pl.pallas_call(
        kernel,
        name="adjoint",
        out_shape=tuple(pltpu.VMEM(shape, bf) for shape in shapes),
        in_specs=[anywhere] * 6 + [pl.BlockSpec(memory_space=pltpu.SMEM), anywhere],
        out_specs=(vmem,) * 4,
        scratch_shapes=[
            pltpu.VMEM((blocks, ROWS, 2 * COL), bf),
            pltpu.VMEM((ROWS, COL), bf),
            pltpu.VMEM((2, ROWS), f32),
            pltpu.VMEM((TOK, COL), bf),
            pltpu.VMEM((TOK, COL), bf),
            pltpu.VMEM((2, DH, TOK), bf),
            pltpu.VMEM((HEADS * COL, COL), bf),
            pltpu.VMEM((NZ * NY, 4, BLK), f32),
            pltpu.VMEM((NZ * NX, 4, BLK), f32),
            pltpu.VMEM((2, TOK, NZ * NX * BLK), bf),
            pltpu.VMEM((2, TOK, NZ * NX * BLK), bf),
            pltpu.VMEM((NZ * (NX - 1), NY, ROWS, COL), bf),
            pltpu.VMEM((NZ, BLK, COL), f32),
            pltpu.VMEM((NZ * (NX - 1), NY, ROWS, COL), bf),
            pltpu.VMEM((NZ * NY, ROWS, COL), bf),
            pltpu.VMEM((NZ * NY, ROWS, COL), bf),
            pltpu.VMEM((HEADS, ROWS, COL), bf),
            pltpu.VMEM((HEADS, ROWS, COL), bf),
            dma((7,)), dma((2,)), dma((NZ,)), dma((NZ,)), dma((NZ * (NX - 1),)), dma((2,)), dma((NZ * (NX - 1),)),
            dma((NZ * (NX - 1),)), dma((NZ,)), dma((1,)),
            dma((NZ * NY,)), dma((NZ * NX,)), dma((NY,)), dma((NZ * NY,)), dma((NZ * NX,)), dma((NZ * (NX - 1),)),
            dma((NY + 1,)), dma((HEADS,)),
        ],
        compiler_params=pltpu.CompilerParams(collective_id=0, has_side_effects=True),
    )(queries, out_grad, attn_out, logsumexp.T, keys, values, obs_counts, query_weight)
    return pl.pallas_call(
        finish,
        name="finish",
        out_shape=tuple(jax.ShapeDtypeStruct(shape, bf) for shape in shapes),
        in_specs=[vmem] * 4,
        out_specs=(anywhere,) * 4,
        scratch_shapes=[dma((4,))],
    )(*[pltpu.with_memory_space_constraint(a, pltpu.VMEM) for a in held])


def solution(mesh):
    in_specs = (
        P("obs", "head"),
        P("obs", "head"),
        P("obs", "head"),
        P("obs", "head"),
        P("obs", "head"),
        P("obs", "head"),
        P("obs"),
        P(None, "head"),
    )
    out_specs = (P("obs", "head"), P("obs", "head"), P("obs", "head"), P("obs", "head"))
    return jax.shard_map(
        on_device, mesh=mesh, in_specs=in_specs, out_specs=out_specs, check_vma=False
    )
```
